8 devices in a mesh: dp: 2 (over z, y), tp: 4 (over x, core).
Axes of the slice: x: 2, y: 2, z: 1, core: 2. Of those that a mesh axis runs over, the one named last changes fastest.
Arguments:
- hidden: bfloat16 [4, 512, 3072], P('dp'), parts along dimension 0
- lengths: int32 [4], P('dp'), parts along dimension 0
- w_query: bfloat16 [2, 3072, 16, 256], P(None, None, 'tp')
- w_key: bfloat16 [2, 3072, 16, 256], P(None, None, 'tp')
- w_value: bfloat16 [2, 3072, 16, 256], P(None, None, 'tp')
- w_out: bfloat16 [2, 16, 256, 3072], P(None, 'tp')
- w_gate: bfloat16 [2, 3072, 24576], P(None, None, 'tp')
- w_up: bfloat16 [2, 3072, 24576], P(None, None, 'tp')
- w_down: bfloat16 [2, 24576, 3072], P(None, 'tp')
- norm_attn: float32 [2, 3072], replicated
- norm_mlp: float32 [2, 3072], replicated
Outputs:
- output 1: bfloat16 [4, 512, 3072], P('dp'), parts along dimension 0
- output 2: bfloat16 [2, 4, 16, 512, 256], P(None, 'dp', 'tp'), parts along dimension 1
- output 3: bfloat16 [2, 4, 16, 512, 256], P(None, 'dp', 'tp'), parts along dimension 1
There are 2 independent parts. The reference program is written for one: setup_inputs(seed, part) draws one part's arguments, and reference() takes and returns one part's arrays. A program takes and returns all parts, laid end to end along the dimension named above; an argument that names none is the same for every part.
All inputs are finite; a program needn't handle non-finite values.
Results may differ from the reference program's by a relative error of at most 0.0179353.
Values are sent between devices in bfloat16 or wider.
A program may use at most 1.25 GiB of HBM per device.

```python
import jax
import jax.numpy as jnp
from jax import lax

BATCH_ROWS = 2
SEQ_LEN = 512
D_MODEL = 3072
N_HEADS = 16
HEAD_DIM = 256
FF_DIM = 24576
LAYER_COUNT = 2
INNER_DIM = N_HEADS * HEAD_DIM
RMS_EPS = 1e-6
ROPE_BASE = 10000.0


def draw_lengths(len_key):
    key_len, key_full = jax.random.split(len_key)
    drawn = jax.random.randint(key_len, (BATCH_ROWS,), 1, SEQ_LEN + 1)
    full_row = jax.random.randint(key_full, (), 0, BATCH_ROWS)
    return jnp.where(jnp.arange(BATCH_ROWS) == full_row, SEQ_LEN, drawn).astype(jnp.int32)


def setup_inputs(seed: int = 0, part: int = 0) -> dict:
    base_key = jax.random.key(seed)
    part_key = jax.random.fold_in(base_key, part)
    hid_key, len_key = jax.random.split(part_key)
    weight_keys = jax.random.split(base_key, 9)

    def normal_bf16(draw_key, shape, fan_in):
        return (jax.random.normal(draw_key, shape, jnp.float32) * fan_in ** -0.5).astype(jnp.bfloat16)

    qkv_shape = (LAYER_COUNT, D_MODEL, N_HEADS, HEAD_DIM)
    return {
        "hidden": jax.random.normal(hid_key, (BATCH_ROWS, SEQ_LEN, D_MODEL), jnp.float32).astype(jnp.bfloat16),
        "lengths": draw_lengths(len_key),
        "w_query": normal_bf16(weight_keys[0], qkv_shape, D_MODEL),
        "w_key": normal_bf16(weight_keys[1], qkv_shape, D_MODEL),
        "w_value": normal_bf16(weight_keys[2], qkv_shape, D_MODEL),
        "w_out": normal_bf16(weight_keys[3], (LAYER_COUNT, N_HEADS, HEAD_DIM, D_MODEL), INNER_DIM),
        "w_gate": normal_bf16(weight_keys[4], (LAYER_COUNT, D_MODEL, FF_DIM), D_MODEL),
        "w_up": normal_bf16(weight_keys[5], (LAYER_COUNT, D_MODEL, FF_DIM), D_MODEL),
        "w_down": normal_bf16(weight_keys[6], (LAYER_COUNT, FF_DIM, D_MODEL), FF_DIM),
        "norm_attn": 0.3 * jax.random.normal(weight_keys[7], (LAYER_COUNT, D_MODEL), jnp.float32),
        "norm_mlp": 0.3 * jax.random.normal(weight_keys[8], (LAYER_COUNT, D_MODEL), jnp.float32),
    }


def rms_norm(x_in, norm_gain):
    x_f32 = x_in.astype(jnp.float32)
    mean_sq = jnp.mean(x_f32 * x_f32, axis=-1, keepdims=True)
    return (x_f32 * lax.rsqrt(mean_sq + RMS_EPS) * (1.0 + norm_gain)).astype(jnp.bfloat16)


def apply_rope(x_in, cos_t, sin_t):
    half_dim = HEAD_DIM // 2
    x_low = x_in[..., :half_dim]
    x_high = x_in[..., half_dim:]
    return jnp.concatenate([x_low * cos_t - x_high * sin_t, x_high * cos_t + x_low * sin_t], axis=-1)


def one_layer(x_in, params, length, cos_t, sin_t):
    w_query, w_key, w_value, w_out, w_gate, w_up, w_down, gain_attn, gain_mlp = params
    normed = rms_norm(x_in, gain_attn)
    query = jnp.dot(normed, w_query.reshape(D_MODEL, INNER_DIM), preferred_element_type=jnp.float32).reshape(SEQ_LEN, N_HEADS, HEAD_DIM)
    keys = jnp.dot(normed, w_key.reshape(D_MODEL, INNER_DIM), preferred_element_type=jnp.float32).reshape(SEQ_LEN, N_HEADS, HEAD_DIM)
    values = jnp.dot(normed, w_value.reshape(D_MODEL, INNER_DIM), preferred_element_type=jnp.float32).astype(jnp.bfloat16).reshape(SEQ_LEN, N_HEADS, HEAD_DIM)
    query_rot = (apply_rope(query, cos_t, sin_t) * HEAD_DIM ** -0.5).astype(jnp.bfloat16)
    key_rot = apply_rope(keys, cos_t, sin_t).astype(jnp.bfloat16)
    scores = jnp.einsum("qhd,khd->hqk", query_rot.astype(jnp.float32), key_rot.astype(jnp.float32))
    positions = jnp.arange(SEQ_LEN)
    allowed = (positions[None, :] <= positions[:, None]) & (positions[None, :] < length)
    scores = jnp.where(allowed[None, :, :], scores, -1e30)
    attn_probs = jax.nn.softmax(scores, axis=-1).astype(jnp.bfloat16)
    attn_out = jnp.einsum("hqk,khd->qhd", attn_probs.astype(jnp.float32), values.astype(jnp.float32)).astype(jnp.bfloat16)
    attn_proj = jnp.dot(attn_out.reshape(SEQ_LEN, INNER_DIM), w_out.reshape(INNER_DIM, D_MODEL), preferred_element_type=jnp.float32)
    mid_state = (x_in.astype(jnp.float32) + attn_proj).astype(jnp.bfloat16)
    normed_mlp = rms_norm(mid_state, gain_mlp)
    gate_pre = jnp.dot(normed_mlp, w_gate, preferred_element_type=jnp.float32)
    up_proj = jnp.dot(normed_mlp, w_up, preferred_element_type=jnp.float32)
    hidden_act = (jax.nn.gelu(gate_pre, approximate=True) * up_proj).astype(jnp.bfloat16)
    down_proj = jnp.dot(hidden_act, w_down, preferred_element_type=jnp.float32)
    out_state = (mid_state.astype(jnp.float32) + down_proj).astype(jnp.bfloat16)
    return out_state, (jnp.swapaxes(key_rot, 0, 1), jnp.swapaxes(values, 0, 1))


def reference(hidden, lengths, w_query, w_key, w_value, w_out, w_gate, w_up, w_down, norm_attn, norm_mlp):
    inv_freq = ROPE_BASE ** (-jnp.arange(HEAD_DIM // 2, dtype=jnp.float32) * (2.0 / HEAD_DIM))
    angles = jnp.arange(SEQ_LEN, dtype=jnp.float32)[:, None] * inv_freq[None, :]
    cos_t = jnp.cos(angles)[:, None, :]
    sin_t = jnp.sin(angles)[:, None, :]
    stacked = (w_query, w_key, w_value, w_out, w_gate, w_up, w_down, norm_attn, norm_mlp)

    def one_row(row_args):
        row_hidden, row_length = row_args

        def layer_step(carry, params):
            return one_layer(carry, params, row_length, cos_t, sin_t)

        return lax.scan(layer_step, row_hidden, stacked)

    out_rows, caches = lax.map(one_row, (hidden, lengths))
    key_rows, value_rows = caches
    return out_rows, jnp.swapaxes(key_rows, 0, 1), jnp.swapaxes(value_rows, 0, 1)
```

```python
import functools

import jax
import jax.numpy as jnp
from jax import lax
from jax.experimental import pallas as pl
from jax.experimental.pallas import tpu as pltpu
from jax.sharding import PartitionSpec as P

RMS_EPS = 1e-6
ROPE_BASE = 10000.0
CORE_SWAP = [(0, 1), (1, 0), (2, 3), (3, 2)]
CHIP_SWAP = [(0, 2), (1, 3), (2, 0), (3, 1)]


def rms_norm(x_in, norm_gain):
    x_f32 = x_in.astype(jnp.float32)
    mean_sq = jnp.mean(x_f32 * x_f32, axis=-1, keepdims=True)
    return (x_f32 * lax.rsqrt(mean_sq + RMS_EPS) * (1.0 + norm_gain)).astype(jnp.bfloat16)


def rope_tables(seq_len, head_dim):
    half_dim = head_dim // 2
    inv_freq = ROPE_BASE ** (-jnp.arange(half_dim, dtype=jnp.float32) * (2.0 / head_dim))
    angles = jnp.arange(seq_len, dtype=jnp.float32)[:, None] * inv_freq[None, :]
    return jnp.cos(angles), jnp.sin(angles)


def attn_kernel(len_ref, q_ref, k_ref, v_ref, cos_ref, sin_ref, o_ref, kc_ref):
    seq, dim = q_ref.shape[1:]
    half = dim // 2
    cos_t, sin_t = cos_ref[...], sin_ref[...]

    def rope(ref):
        lo, hi = ref[0, :, :half], ref[0, :, half:]
        return jnp.concatenate([lo * cos_t - hi * sin_t, hi * cos_t + lo * sin_t], axis=-1)

    qr = (rope(q_ref) * (dim ** -0.5)).astype(jnp.bfloat16)
    kr = rope(k_ref).astype(jnp.bfloat16)
    kc_ref[0] = kr
    scores = lax.dot_general(qr, kr, (((1,), (1,)), ((), ())), preferred_element_type=jnp.float32)
    row = lax.broadcasted_iota(jnp.int32, (seq, seq), 0)
    col = lax.broadcasted_iota(jnp.int32, (seq, seq), 1)
    scores = jnp.where((col <= row) & (col < len_ref[0]), scores, -1e30)
    p = jnp.exp(scores - jnp.max(scores, axis=-1, keepdims=True))
    p = p / jnp.sum(p, axis=-1, keepdims=True)
    o = jnp.dot(p.astype(jnp.bfloat16), v_ref[0], preferred_element_type=jnp.float32)
    o_ref[...] = o.astype(jnp.bfloat16)


def attention(length, q, k, v, cos_t, sin_t):
    heads, seq, dim = q.shape
    per_head = pl.BlockSpec((1, seq, dim), lambda h: (h, 0, 0))
    table = pl.BlockSpec((seq, dim // 2), lambda h: (0, 0))
    return pl.pallas_call(
        attn_kernel,
        grid=(heads,),
        in_specs=[pl.BlockSpec(memory_space=pltpu.SMEM), per_head, per_head, per_head, table, table],
        out_specs=[pl.BlockSpec((seq, dim), lambda h: (0, h)), per_head],
        out_shape=[
            jax.ShapeDtypeStruct((seq, heads * dim), jnp.bfloat16),
            jax.ShapeDtypeStruct((heads, seq, dim), jnp.bfloat16),
        ],
        cost_estimate=pl.CostEstimate(
            flops=4 * heads * seq * seq * dim, bytes_accessed=12 * heads * seq * dim, transcendentals=heads * seq * seq
        ),
    )(length, q, k, v, cos_t, sin_t)


def reduce_into(x, part, core):
    half = x.shape[0] // 2
    mine = lax.dynamic_slice_in_dim(part, core * half, half, 0)
    other = lax.dynamic_slice_in_dim(part, (1 - core) * half, half, 0)
    got = lax.ppermute(other, "tp", CORE_SWAP)
    chip_sum = (mine.astype(jnp.float32) + got.astype(jnp.float32)).astype(jnp.bfloat16)
    far_sum = lax.ppermute(chip_sum, "tp", CHIP_SWAP)
    x_mine = lax.dynamic_slice_in_dim(x, core * half, half, 0)
    x_mine = (x_mine.astype(jnp.float32) + (chip_sum.astype(jnp.float32) + far_sum.astype(jnp.float32))).astype(jnp.bfloat16)
    x_other = lax.ppermute(x_mine, "tp", CORE_SWAP)
    return jnp.where(core == 0, jnp.concatenate([x_mine, x_other]), jnp.concatenate([x_other, x_mine]))


def solution(mesh):
    head_cols = P(None, None, "tp", None)
    head_rows = P(None, "tp", None, None)
    ff_cols = P(None, None, "tp")
    ff_rows = P(None, "tp", None)
    f32 = jnp.float32

    def shard_body(hidden, lengths, w_query, w_key, w_value, w_out, w_gate, w_up, w_down, norm_attn, norm_mlp):
        core = lax.axis_index("tp") % 2
        n_layers, _, heads, dim = w_query.shape
        prompts, seq, model = hidden.shape
        cos_t, sin_t = rope_tables(seq, dim)

        def attn_part(x, b, l):
            a = rms_norm(x, norm_attn[l])
            q = jnp.einsum("so,ojf->jsf", a, w_query[l], preferred_element_type=f32)
            k = jnp.einsum("so,ojf->jsf", a, w_key[l], preferred_element_type=f32)
            v = jnp.einsum("so,ojf->jsf", a, w_value[l], preferred_element_type=f32).astype(jnp.bfloat16)
            o, kr = attention(lengths[b][None], q, k, v, cos_t, sin_t)
            part = jnp.dot(o, w_out[l].reshape(heads * dim, model), preferred_element_type=f32).astype(jnp.bfloat16)
            return part, kr, v

        def mlp_part(x, l):
            a = rms_norm(x, norm_mlp[l])
            g = jnp.dot(a, w_gate[l], preferred_element_type=f32)
            u = jnp.dot(a, w_up[l], preferred_element_type=f32)
            m = (jax.nn.gelu(g, approximate=True) * u).astype(jnp.bfloat16)
            return jnp.dot(m, w_down[l], preferred_element_type=f32).astype(jnp.bfloat16)

        xs = [hidden[b] for b in range(prompts)]
        keys, values = [], []
        for l in range(n_layers):
            for b in range(prompts):
                part, kr, v = attn_part(xs[b], b, l)
                keys.append(kr)
                values.append(v)
                xs[b] = reduce_into(xs[b], part, core)
            for b in range(prompts):
                xs[b] = reduce_into(xs[b], mlp_part(xs[b], l), core)
        cache = lambda parts: jnp.stack(parts).reshape(n_layers, prompts, heads, seq, dim)
        return jnp.stack(xs), cache(keys), cache(values)

    return jax.shard_map(
        shard_body,
        mesh=mesh,
        in_specs=(P("dp"), P("dp"), head_cols, head_cols, head_cols, head_rows, ff_cols, ff_cols, ff_rows, P(), P()),
        out_specs=(P("dp"), P(None, "dp", "tp"), P(None, "dp", "tp")),
        check_vma=False,
    )
```

```python
import functools

import jax
import jax.numpy as jnp
from jax import lax
from jax.experimental import pallas as pl
from jax.experimental.pallas import tpu as pltpu
from jax.sharding import PartitionSpec as P

RMS_EPS = 1e-6
ROPE_BASE = 10000.0
CORE_SWAP = [(0, 1), (1, 0), (2, 3), (3, 2)]
CHIP_SWAP = [(0, 2), (1, 3), (2, 0), (3, 1)]


def rms_norm(x_in, norm_gain):
    x_f32 = x_in.astype(jnp.float32)
    mean_sq = jnp.mean(x_f32 * x_f32, axis=-1, keepdims=True)
    return (x_f32 * lax.rsqrt(mean_sq + RMS_EPS) * (1.0 + norm_gain)).astype(jnp.bfloat16)


def rope_tables(seq_len, head_dim):
    half_dim = head_dim // 2
    inv_freq = ROPE_BASE ** (-jnp.arange(half_dim, dtype=jnp.float32) * (2.0 / head_dim))
    angles = jnp.arange(seq_len, dtype=jnp.float32)[:, None] * inv_freq[None, :]
    return jnp.cos(angles), jnp.sin(angles)


def attn_kernel(len_ref, q_ref, k_ref, v_ref, cos_ref, sin_ref, o_ref, kc_ref):
    seq, dim = q_ref.shape[1:]
    half = dim // 2
    cos_t, sin_t = cos_ref[...], sin_ref[...]

    def rope(ref):
        lo, hi = ref[0, :, :half], ref[0, :, half:]
        return jnp.concatenate([lo * cos_t - hi * sin_t, hi * cos_t + lo * sin_t], axis=-1)

    qr = (rope(q_ref) * (dim ** -0.5)).astype(jnp.bfloat16)
    kr = rope(k_ref).astype(jnp.bfloat16)
    kc_ref[0] = kr
    scores = lax.dot_general(qr, kr, (((1,), (1,)), ((), ())), preferred_element_type=jnp.float32)
    row = lax.broadcasted_iota(jnp.int32, (seq, seq), 0)
    col = lax.broadcasted_iota(jnp.int32, (seq, seq), 1)
    scores = jnp.where((col <= row) & (col < len_ref[0]), scores, -1e30)
    p = jnp.exp(scores - jnp.max(scores, axis=-1, keepdims=True))
    p = p / jnp.sum(p, axis=-1, keepdims=True)
    o = jnp.dot(p.astype(jnp.bfloat16), v_ref[0], preferred_element_type=jnp.float32)
    o_ref[...] = o.astype(jnp.bfloat16)


def attention(length, q, k, v, cos_t, sin_t):
    heads, seq, dim = q.shape
    per_head = pl.BlockSpec((1, seq, dim), lambda h: (h, 0, 0))
    table = pl.BlockSpec((seq, dim // 2), lambda h: (0, 0))
    return pl.pallas_call(
        attn_kernel,
        grid=(heads,),
        in_specs=[pl.BlockSpec(memory_space=pltpu.SMEM), per_head, per_head, per_head, table, table],
        out_specs=[pl.BlockSpec((seq, dim), lambda h: (0, h)), per_head],
        out_shape=[
            jax.ShapeDtypeStruct((seq, heads * dim), jnp.bfloat16),
            jax.ShapeDtypeStruct((heads, seq, dim), jnp.bfloat16),
        ],
        cost_estimate=pl.CostEstimate(
            flops=4 * heads * seq * seq * dim, bytes_accessed=12 * heads * seq * dim, transcendentals=heads * seq * seq
        ),
    )(length, q, k, v, cos_t, sin_t)


GU_COLS = 512
DOWN_COLS = 512


def norm_rows(x_ref, gain_ref, a_ref):
    rows = x_ref.shape[0]
    step = 64
    gain = 1.0 + gain_ref[...]

    def body(i, _):
        at = pl.ds(pl.multiple_of(i * step, step), step)
        x = x_ref[at, :].astype(jnp.float32)
        mean_sq = jnp.mean(x * x, axis=-1, keepdims=True)
        a_ref[at, :] = (x * lax.rsqrt(mean_sq + RMS_EPS) * gain).astype(jnp.bfloat16)
        return 0

    lax.fori_loop(0, rows // step, body, 0)


def mlp_kernel(layer, x_hbm, gain_ref, wg_hbm, wu_hbm, wd_hbm, out_ref, x_vm, a_vm, m_vm, wg_vm, wu_vm, wd_vm, g_vm, u_vm, x_sem, g_sem, u_sem, d_sem):
    model, width = wg_hbm.shape[1:]
    n_gu, n_down = width // GU_COLS, model // DOWN_COLS

    def gu_copies(t, slot):
        cols = pl.ds(pl.multiple_of(t * GU_COLS, GU_COLS), GU_COLS)
        return (
            pltpu.make_async_copy(wg_hbm.at[layer, :, cols], wg_vm.at[slot], g_sem.at[slot]),
            pltpu.make_async_copy(wu_hbm.at[layer, :, cols], wu_vm.at[slot], u_sem.at[slot]),
        )

    def down_copy(t, slot):
        cols = pl.ds(pl.multiple_of(t * DOWN_COLS, DOWN_COLS), DOWN_COLS)
        return pltpu.make_async_copy(wd_hbm.at[layer, :, cols], wd_vm.at[slot], d_sem.at[slot])

    x_copy = pltpu.make_async_copy(x_hbm, x_vm, x_sem)
    x_copy.start()
    for c in gu_copies(0, 0):
        c.start()
    x_copy.wait()
    norm_rows(x_vm, gain_ref, a_vm)

    def finish(t, slot):
        cols = pl.ds(pl.multiple_of(t * GU_COLS, GU_COLS), GU_COLS)
        m_vm[:, cols] = (jax.nn.gelu(g_vm[slot], approximate=True) * u_vm[slot]).astype(jnp.bfloat16)

    def one(t, slot, first):
        for c in gu_copies(t, slot):
            c.wait()

        @pl.when(t + 1 < n_gu)
        def _():
            for c in gu_copies(t + 1, 1 - slot):
                c.start()

        if not first:
            finish(t - 1, 1 - slot)
        g_vm[slot] = jnp.dot(a_vm[...], wg_vm[slot], preferred_element_type=jnp.float32)
        u_vm[slot] = jnp.dot(a_vm[...], wu_vm[slot], preferred_element_type=jnp.float32)

    one(0, 0, True)
    down_copy(0, 0).start()

    def pair(i, _):
        one(2 * i + 1, 1, False)
        one(2 * i + 2, 0, False)
        return 0

    lax.fori_loop(0, (n_gu - 2) // 2, pair, 0)
    one(n_gu - 1, 1, False)
    finish(n_gu - 1, 1)

    def down(t, slot):
        down_copy(t, slot).wait()

        @pl.when(t + 1 < n_down)
        def _():
            down_copy(t + 1, 1 - slot).start()

        cols = pl.ds(pl.multiple_of(t * DOWN_COLS, DOWN_COLS), DOWN_COLS)
        out_ref[:, cols] = jnp.dot(m_vm[...], wd_vm[slot], preferred_element_type=jnp.float32).astype(jnp.bfloat16)

    def down_pair(i, _):
        down(2 * i, 0)
        down(2 * i + 1, 1)
        return 0

    lax.fori_loop(0, n_down // 2, down_pair, 0)


def mlp(x, gain, wg, wu, wd, layer):
    rows, model = x.shape
    width = wg.shape[2]
    anywhere = pl.BlockSpec(memory_space=pl.ANY)
    bf16, f32 = jnp.bfloat16, jnp.float32
    return pl.pallas_call(
        functools.partial(mlp_kernel, layer),
        in_specs=[anywhere, pl.BlockSpec(memory_space=pltpu.VMEM), anywhere, anywhere, anywhere],
        out_specs=pl.BlockSpec(memory_space=pltpu.VMEM),
        out_shape=jax.ShapeDtypeStruct((rows, model), bf16),
        scratch_shapes=[
            pltpu.VMEM((rows, model), bf16),
            pltpu.VMEM((rows, model), bf16),
            pltpu.VMEM((rows, width), bf16),
            pltpu.VMEM((2, model, GU_COLS), bf16),
            pltpu.VMEM((2, model, GU_COLS), bf16),
            pltpu.VMEM((2, width, DOWN_COLS), bf16),
            pltpu.VMEM((2, rows, GU_COLS), f32),
            pltpu.VMEM((2, rows, GU_COLS), f32),
            pltpu.SemaphoreType.DMA,
            pltpu.SemaphoreType.DMA((2,)),
            pltpu.SemaphoreType.DMA((2,)),
            pltpu.SemaphoreType.DMA((2,)),
        ],
        compiler_params=pltpu.CompilerParams(vmem_limit_bytes=60 * 1024 * 1024),
        cost_estimate=pl.CostEstimate(
            flops=6 * rows * model * width, bytes_accessed=6 * model * width + 4 * rows * model, transcendentals=rows * width
        ),
    )(x, gain, wg, wu, wd)


def reduce_into(x, part, core):
    half = x.shape[0] // 2
    mine = lax.dynamic_slice_in_dim(part, core * half, half, 0)
    other = lax.dynamic_slice_in_dim(part, (1 - core) * half, half, 0)
    got = lax.ppermute(other, "tp", CORE_SWAP)
    chip_sum = (mine.astype(jnp.float32) + got.astype(jnp.float32)).astype(jnp.bfloat16)
    far_sum = lax.ppermute(chip_sum, "tp", CHIP_SWAP)
    x_mine = lax.dynamic_slice_in_dim(x, core * half, half, 0)
    x_mine = (x_mine.astype(jnp.float32) + (chip_sum.astype(jnp.float32) + far_sum.astype(jnp.float32))).astype(jnp.bfloat16)
    x_other = lax.ppermute(x_mine, "tp", CORE_SWAP)
    return jnp.where(core == 0, jnp.concatenate([x_mine, x_other]), jnp.concatenate([x_other, x_mine]))


def solution(mesh):
    head_cols = P(None, None, "tp", None)
    head_rows = P(None, "tp", None, None)
    ff_cols = P(None, None, "tp")
    ff_rows = P(None, "tp", None)
    f32 = jnp.float32

    def shard_body(hidden, lengths, w_query, w_key, w_value, w_out, w_gate, w_up, w_down, norm_attn, norm_mlp):
        core = lax.axis_index("tp") % 2
        n_layers, _, heads, dim = w_query.shape
        prompts, seq, model = hidden.shape
        cos_t, sin_t = rope_tables(seq, dim)

        def attn_part(x, b, l):
            a = rms_norm(x, norm_attn[l])
            q = jnp.einsum("so,ojf->jsf", a, w_query[l], preferred_element_type=f32)
            k = jnp.einsum("so,ojf->jsf", a, w_key[l], preferred_element_type=f32)
            v = jnp.einsum("so,ojf->jsf", a, w_value[l], preferred_element_type=f32).astype(jnp.bfloat16)
            o, kr = attention(lengths[b][None], q, k, v, cos_t, sin_t)
            part = jnp.dot(o, w_out[l].reshape(heads * dim, model), preferred_element_type=f32).astype(jnp.bfloat16)
            return part, kr, v

        def mlp_part(x, l):
            return mlp(x, norm_mlp[l][None], w_gate, w_up, w_down, l)

        xs = [hidden[b] for b in range(prompts)]
        keys, values = [], []
        for l in range(n_layers):
            for b in range(prompts):
                part, kr, v = attn_part(xs[b], b, l)
                keys.append(kr)
                values.append(v)
                xs[b] = reduce_into(xs[b], part, core)
            for b in range(prompts):
                xs[b] = reduce_into(xs[b], mlp_part(xs[b], l), core)
        cache = lambda parts: jnp.stack(parts).reshape(n_layers, prompts, heads, seq, dim)
        return jnp.stack(xs), cache(keys), cache(values)

    return jax.shard_map(
        shard_body,
        mesh=mesh,
        in_specs=(P("dp"), P("dp"), head_cols, head_cols, head_cols, head_rows, ff_cols, ff_cols, ff_rows, P(), P()),
        out_specs=(P("dp"), P(None, "dp", "tp"), P(None, "dp", "tp")),
        check_vma=False,
    )
```

```python
import jax
import jax.numpy as jnp
from jax import lax
from jax.experimental import pallas as pl
from jax.experimental.pallas import tpu as pltpu
from jax.sharding import PartitionSpec as P

RMS_EPS = 1e-6
ROPE_BASE = 10000.0
TILE = 512
NORM_ROWS = 64
F32, BF16 = jnp.float32, jnp.bfloat16


def rope_tables(seq_len, head_dim):
    half_dim = head_dim // 2
    inv_freq = ROPE_BASE ** (-jnp.arange(half_dim, dtype=F32) * (2.0 / head_dim))
    angles = jnp.arange(seq_len, dtype=F32)[:, None] * inv_freq[None, :]
    return jnp.cos(angles), jnp.sin(angles)


def block(i, size):
    return pl.ds(pl.multiple_of(i * size, size), size)


def kernel(
    len_ref, hidden, w_query, w_key, w_value, w_out, w_gate, w_up, w_down, gain_attn, gain_mlp, cos_ref, sin_ref,
    h_out, k_cache, v_cache,
    x, a, m, wa, wb, raw, ga, ub, part, recv1, recv2,
    x_sem, wa_sem, wb_sem, raw_sem, wo_sem, kc_sem, vc_sem, s1, r1, s2, r2, s3, r3,
):
    n_layers, model, heads, dim = w_query.shape
    prompts, seq, _ = hidden.shape
    inner = heads * dim
    n_gu = w_gate.shape[2] // TILE
    n_down = model // TILE
    half = seq // 2
    n_raw = raw_sem.shape[0]
    raw_rows = model // n_raw
    half_dim = dim // 2

    me = lax.axis_index("tp")
    core = lax.rem(me, 2)
    peer = {"tp": me + 1 - 2 * core}
    far = {"tp": lax.rem(me + 2, 4)}
    own = block(core, half)
    other = block(1 - core, half)

    def remote(src, dst, send_sem, recv_sem, device):
        return pltpu.make_async_remote_copy(src, dst, send_sem, recv_sem, device_id=device, device_id_type=pl.DeviceIdType.MESH)

    def send_part(b, t):
        c = block(t, TILE)
        return remote(part.at[b, other, c], recv1.at[b, :, c], s1.at[b, t], r1.at[b, t], peer)

    def send_far(b, stage, t):
        c = block(t, TILE)
        return remote(part.at[b, own, c], recv2.at[stage, b, :, c], s2.at[b, t], r2.at[stage, b, t], far)

    def send_x(b, t):
        c = block(t, TILE)
        return remote(x.at[b, own, c], x.at[b, own, c], s3.at[b, t], r3.at[b, t], peer)

    def chip_add(b, stage, t):
        c = block(t, TILE)
        send_part(b, t).wait_recv()
        part[b, own, c] = (part[b, own, c].astype(F32) + recv1[b, :, c].astype(F32)).astype(BF16)
        send_far(b, stage, t).start()

    def finish_sum(b, stage):
        def body(t, _):
            c = block(t, TILE)
            send_far(b, stage, t).wait_recv()
            total = part[b, own, c].astype(F32) + recv2[stage, b, :, c].astype(F32)
            x[b, own, c] = (x[b, own, c].astype(F32) + total).astype(BF16)
            send_x(b, t).start()
            return 0

        lax.fori_loop(0, n_down, body, 0)

    def finish_wait(b, stage):
        def body(t, _):
            send_part(b, t).wait_send()
            send_far(b, stage, t).wait_send()
            send_x(b, t).wait()
            return 0

        lax.fori_loop(0, n_down, body, 0)

    def norm(b, gain_ref, layer):
        gain = 1.0 + gain_ref[pl.ds(layer, 1), :]

        def body(i, _):
            rows = block(i, NORM_ROWS)
            v = x[b, rows, :].astype(F32)
            mean_sq = jnp.mean(v * v, axis=-1, keepdims=True)
            a[rows, :] = (v * lax.rsqrt(mean_sq + RMS_EPS) * gain).astype(BF16)
            return 0

        lax.fori_loop(0, seq // NORM_ROWS, body, 0)

    def raw_copy(w, layer, c):
        rows = pl.ds(c * raw_rows, raw_rows)
        return pltpu.make_async_copy(w.at[layer, rows], raw.at[rows], raw_sem.at[c])

    def raw_start(w, layer):
        for c in range(n_raw):
            raw_copy(w, layer, c).start()

    def raw_wait(w, layer):
        for c in range(n_raw):
            raw_copy(w, layer, c).wait()

    def relayout(slot):
        for c in range(n_raw):
            rows = pl.ds(c * raw_rows, raw_rows)
            v = raw[rows].reshape(raw_rows, inner)
            wa[slot, rows, :] = v[:, :TILE]
            wb[slot, rows, :] = v[:, TILE:]

    def out_copy(layer, t):
        dst = (wa if t < 3 else wb).at[1, pl.ds((t % 3) * inner, inner), :]
        return pltpu.make_async_copy(w_out.at[layer, :, pl.ds(t * TILE, TILE)], dst, wo_sem.at[t])

    def gu_copies(layer, t, slot):
        c = block(t, TILE)
        return (
            pltpu.make_async_copy(w_gate.at[layer, :, c], wa.at[slot], wa_sem.at[slot]),
            pltpu.make_async_copy(w_up.at[layer, :, c], wb.at[slot], wb_sem.at[slot]),
        )

    def down_copies(layer, t, slot):
        c = block(t, TILE)
        return (
            pltpu.make_async_copy(w_down.at[layer, pl.ds(0, model), c], wa.at[slot], wa_sem.at[slot]),
            pltpu.make_async_copy(w_down.at[layer, pl.ds(model, model), c], wb.at[slot], wb_sem.at[slot]),
        )

    def start(copies):
        for c in copies:
            c.start()

    def wait(copies):
        for c in copies:
            c.wait()

    def dot(p, q):
        return jnp.dot(p, q, preferred_element_type=F32)

    def cache_copies(layer, b, h):
        return (
            pltpu.make_async_copy(m.at[:, block(heads + h, dim)], k_cache.at[layer, b, h], kc_sem.at[h]),
            pltpu.make_async_copy(m.at[:, block(h, dim)], v_cache.at[layer, b, h], vc_sem.at[h]),
        )

    def head(b, i, j):
        h = 2 * i + j
        lanes = slice(j * dim, (j + 1) * dim)
        cos_t, sin_t = cos_ref[...], sin_ref[...]

        def rope(v):
            lo, hi = v[:, :half_dim], v[:, half_dim:]
            return jnp.concatenate([lo * cos_t - hi * sin_t, hi * cos_t + lo * sin_t], axis=-1)

        q = (rope(ga[i, :, lanes]) * (dim ** -0.5)).astype(BF16)
        k = rope(ub[i, :, lanes]).astype(BF16)
        m[:, block(heads + h, dim)] = k
        for r in range(2):
            keys = (r + 1) * half
            v = m[pl.ds(0, keys), block(h, dim)]
            scores = lax.dot_general(q[r * half:keys], k[:keys], (((1,), (1,)), ((), ())), preferred_element_type=F32)
            row = r * half + lax.broadcasted_iota(jnp.int32, (half, keys), 0)
            col = lax.broadcasted_iota(jnp.int32, (half, keys), 1)
            scores = jnp.where((col <= row) & (col < len_ref[b]), scores, -1e30)
            p = jnp.exp(scores - jnp.max(scores, axis=-1, keepdims=True))
            p = (p * (1.0 / jnp.sum(p, axis=-1, keepdims=True))).astype(BF16)
            m[pl.ds(r * half, half), block(2 * heads + h, dim)] = dot(p, v).astype(BF16)

    def attn_phase(layer, b):
        norm(b, gain_attn, layer)
        raw_wait(w_query, layer)
        relayout(0)
        raw_start(w_key, layer)
        ga[0] = dot(a[...], wa[0])
        raw_wait(w_key, layer)
        relayout(1)
        ga[1] = dot(a[...], wb[0])
        raw_start(w_value, layer)
        ub[0] = dot(a[...], wa[1])
        raw_wait(w_value, layer)
        relayout(0)
        ub[1] = dot(a[...], wb[1])
        for t in range(n_down):
            out_copy(layer, t).start()

        @pl.when(b == 0)
        def _():
            raw_start(w_query, layer)

        m[:, pl.ds(0, TILE)] = dot(a[...], wa[0]).astype(BF16)
        m[:, pl.ds(TILE, TILE)] = dot(a[...], wb[0]).astype(BF16)

        @pl.when(b == 1)
        def _():
            start(gu_copies(layer, 0, 0))

        def two_heads(i, _):
            head(b, i, 0)
            head(b, i, 1)
            start(cache_copies(layer, b, 2 * i))
            start(cache_copies(layer, b, 2 * i + 1))
            return 0

        lax.fori_loop(0, heads // 2, two_heads, 0)

        @pl.when((b == 0) & (layer > 0))
        def _():
            finish_sum(1, 1)

        for t in range(n_down):
            out_copy(layer, t).wait()
        o_cols = pl.ds(2 * inner, inner)

        def project(i, _):
            @pl.when(i > 0)
            def _():
                send_part(b, i - 1).start()
                send_part(b, i + 2).start()

            part[b, :, block(i, TILE)] = dot(m[:, o_cols], wa[1, block(i, inner), :]).astype(BF16)
            part[b, :, block(i + 3, TILE)] = dot(m[:, o_cols], wb[1, block(i, inner), :]).astype(BF16)
            return 0

        lax.fori_loop(0, 3, project, 0)
        for h in range(heads):
            wait(cache_copies(layer, b, h))
        send_part(b, 2).start()
        send_part(b, 5).start()
        for t in (0, 3, 1, 4, 2, 5):
            chip_add(b, 0, t)

        @pl.when((b == 0) & (layer > 0))
        def _():
            finish_wait(1, 1)

        @pl.when(b == 1)
        def _():
            finish_sum(0, 0)
            finish_wait(0, 0)

    def mlp_phase(layer, b):
        @pl.when((b == 1) & (layer + 1 < n_layers))
        def _():
            raw_start(w_query, layer + 1)

        norm(b, gain_mlp, layer)

        def activate(t, slot):
            m[:, block(t, TILE)] = (jax.nn.gelu(ga[slot], approximate=True) * ub[slot]).astype(BF16)

        def gate_up(t, slot):
            wait(gu_copies(layer, t, slot))

            @pl.when(t + 1 < n_gu)
            def _():
                start(gu_copies(layer, t + 1, 1 - slot))

            @pl.when(t + 1 == n_gu)
            def _():
                start(down_copies(layer, 0, 1 - slot))

            activate(lax.rem(t + n_gu - 1, n_gu), 1 - slot)
            ga[slot] = dot(a[...], wa[slot])
            ub[slot] = dot(a[...], wb[slot])

        def gate_up_pair(i, _):
            gate_up(2 * i, 0)
            gate_up(2 * i + 1, 1)
            return 0

        lax.fori_loop(0, n_gu // 2, gate_up_pair, 0)
        activate(n_gu - 1, 1)
        finish_sum(1 - b, b)

        def down(t, slot):
            wait(down_copies(layer, t, slot))

            @pl.when(t + 1 < n_down)
            def _():
                start(down_copies(layer, t + 1, 1 - slot))

            @pl.when((t + 1 == n_down) & (b == 0))
            def _():
                start(gu_copies(layer, 0, 1 - slot))

            @pl.when(t > 0)
            def _():
                send_part(b, t - 1).start()

            @pl.when(t > 1)
            def _():
                chip_add(b, 1, t - 2)

            part[b, :, block(t, TILE)] = (
                dot(m[:, pl.ds(0, model)], wa[slot]) + dot(m[:, pl.ds(model, model)], wb[slot])
            ).astype(BF16)

        def down_pair(i, _):
            down(2 * i, 0)
            down(2 * i + 1, 1)
            return 0

        lax.fori_loop(0, n_down // 2, down_pair, 0)
        finish_wait(1 - b, b)
        send_part(b, n_down - 1).start()
        chip_add(b, 1, n_down - 2)
        chip_add(b, 1, n_down - 1)

    hidden_copies = [pltpu.make_async_copy(hidden.at[b], x.at[b], x_sem.at[b]) for b in range(prompts)]
    start(hidden_copies)
    raw_start(w_query, 0)
    barrier = pltpu.get_barrier_semaphore()
    for device in (peer, far):
        pl.semaphore_signal(barrier, inc=1, device_id=device, device_id_type=pl.DeviceIdType.MESH)
    wait(hidden_copies)
    pl.semaphore_wait(barrier, 2)

    def layer_step(layer, _):
        def attn_step(b, _):
            attn_phase(layer, b)
            return 0

        def mlp_step(b, _):
            mlp_phase(layer, b)
            return 0

        lax.fori_loop(0, prompts, attn_step, 0)
        lax.fori_loop(0, prompts, mlp_step, 0)
        return 0

    lax.fori_loop(0, n_layers, layer_step, 0)
    out_copies = [pltpu.make_async_copy(x.at[b], h_out.at[b], x_sem.at[b]) for b in range(prompts)]
    out_copies[0].start()
    finish_sum(1, 1)
    finish_wait(1, 1)
    out_copies[1].start()
    wait(out_copies)


def solution(mesh):
    head_cols = P(None, None, "tp", None)
    head_rows = P(None, "tp", None, None)
    ff_cols = P(None, None, "tp")
    ff_rows = P(None, "tp", None)

    def shard_body(hidden, lengths, w_query, w_key, w_value, w_out, w_gate, w_up, w_down, norm_attn, norm_mlp):
        n_layers, model, heads, dim = w_query.shape
        prompts, seq, _ = hidden.shape
        width = w_gate.shape[2]
        inner = heads * dim
        n_down = model // TILE
        half = seq // 2
        cos_t, sin_t = rope_tables(seq, dim)
        anywhere = pl.BlockSpec(memory_space=pl.ANY)
        vmem = pl.BlockSpec(memory_space=pltpu.VMEM)
        dma = pltpu.SemaphoreType.DMA
        cache = jax.ShapeDtypeStruct((n_layers, prompts, heads, seq, dim), BF16)
        return pl.pallas_call(
            kernel,
            in_specs=[pl.BlockSpec(memory_space=pltpu.SMEM)] + [anywhere] * 8 + [vmem] * 4,
            out_specs=[anywhere] * 3,
            out_shape=[jax.ShapeDtypeStruct(hidden.shape, BF16), cache, cache],
            scratch_shapes=[
                pltpu.VMEM((prompts, seq, model), BF16),
                pltpu.VMEM((seq, model), BF16),
                pltpu.VMEM((seq, width), BF16),
                pltpu.VMEM((2, model, TILE), BF16),
                pltpu.VMEM((2, model, TILE), BF16),
                pltpu.VMEM((model, heads, dim), BF16),
                pltpu.VMEM((2, seq, TILE), F32),
                pltpu.VMEM((2, seq, TILE), F32),
                pltpu.VMEM((prompts, seq, model), BF16),
                pltpu.VMEM((prompts, half, model), BF16),
                pltpu.VMEM((2, prompts, half, model), BF16),
                dma((prompts,)), dma((2,)), dma((2,)), dma((4,)), dma((n_down,)), dma((heads,)), dma((heads,)),
                dma((prompts, n_down)), dma((prompts, n_down)), dma((prompts, n_down)), dma((2, prompts, n_down)),
                dma((prompts, n_down)), dma((prompts, n_down)),
            ],
            compiler_params=pltpu.CompilerParams(
                collective_id=0, has_side_effects=True, vmem_limit_bytes=63 * 1024 * 1024
            ),
        )(
            lengths, hidden, w_query, w_key, w_value, w_out.reshape(n_layers, inner, model), w_gate, w_up, w_down,
            norm_attn, norm_mlp, cos_t, sin_t,
        )

    return jax.shard_map(
        shard_body,
        mesh=mesh,
        in_specs=(P("dp"), P("dp"), head_cols, head_cols, head_cols, head_rows, ff_cols, ff_cols, ff_rows, P(), P()),
        out_specs=(P("dp"), P(None, "dp", "tp"), P(None, "dp", "tp")),
        check_vma=False,
    )
```

```python
import jax
import jax.numpy as jnp
import numpy as np
from jax import lax
from jax.experimental import pallas as pl
from jax.experimental.pallas import tpu as pltpu
from jax.sharding import PartitionSpec as P

RMS_EPS = 1e-6
ROPE_BASE = 10000.0
TILE = 512
NORM_ROWS = 64
ACT_ROWS = 16
SPREAD_ROWS = 96
F32, BF16 = jnp.float32, jnp.bfloat16


def rope_tables(seq_len, head_dim):
    half_dim = head_dim // 2
    inv_freq = np.float32(ROPE_BASE) ** (-np.arange(half_dim, dtype=np.float32) * np.float32(2.0 / head_dim))
    angles = np.arange(seq_len, dtype=np.float32)[:, None] * inv_freq[None, :].astype(np.float32)
    return np.cos(angles).astype(np.float32), np.sin(angles).astype(np.float32)


def block(i, size):
    return pl.ds(pl.multiple_of(i * size, size), size)


def kernel(
    len_ref, hidden, w_query, w_key, w_value, w_out, w_gate, w_up, w_down, gains, cos_ref, sin_ref,
    h_out0, h_out1, k_cache, v_cache,
    x, a, m, wa, wb, raw, ga, ub, part, recv1, recv2,
    x_sem, wa_sem, wb_sem, raw_sem, wo_sem, kc_sem, vc_sem, s1, r1, s2, r2, s3, r3,
):
    n_layers, model, heads, dim = w_query.shape
    prompts, seq, _ = hidden.shape
    inner = heads * dim
    n_gu = w_gate.shape[2] // TILE
    n_down = model // TILE
    half = seq // 2
    n_raw = raw_sem.shape[0]
    raw_rows = model // n_raw
    half_dim = dim // 2

    me = lax.axis_index("tp")
    core = lax.rem(me, 2)
    peer = {"tp": me + 1 - 2 * core}
    far = {"tp": lax.rem(me + 2, 4)}
    own = block(core, half)
    other = block(1 - core, half)

    def remote(src, dst, send_sem, recv_sem, device):
        return pltpu.make_async_remote_copy(src, dst, send_sem, recv_sem, device_id=device, device_id_type=pl.DeviceIdType.MESH)

    def send_part(b, t):
        c = block(t, TILE)
        return remote(part.at[b, other, c], recv1.at[b, :, c], s1.at[b, t], r1.at[b, t], peer)

    def send_far(b, stage, t):
        c = block(t, TILE)
        return remote(part.at[b, own, c], recv2.at[stage, b, :, c], s2.at[b, t], r2.at[stage, b, t], far)

    def send_x(b, t):
        c = block(t, TILE)
        return remote(x.at[b, own, c], x.at[b, own, c], s3.at[b, t], r3.at[b, t], peer)

    def chip_add(b, stage, t):
        c = block(t, TILE)
        send_part(b, t).wait_recv()
        part[b, own, c] = (part[b, own, c].astype(F32) + recv1[b, :, c].astype(F32)).astype(BF16)
        send_far(b, stage, t).start()

    def finish_sum(b, stage):
        def body(t, _):
            c = block(t, TILE)
            send_far(b, stage, t).wait_recv()
            total = part[b, own, c].astype(F32) + recv2[stage, b, :, c].astype(F32)
            x[b, own, c] = (x[b, own, c].astype(F32) + total).astype(BF16)
            send_x(b, t).start()
            return 0

        lax.fori_loop(0, n_down, body, 0)

    def finish_wait(b, stage):
        def body(t, _):
            send_part(b, t).wait_send()
            send_far(b, stage, t).wait_send()
            send_x(b, t).wait()
            return 0

        lax.fori_loop(0, n_down, body, 0)

    def norm_rows(b, which, rows):
        v = x[b, rows, :].astype(F32)
        mean_sq = jnp.mean(v * v, axis=-1, keepdims=True)
        a[rows, :] = (v * lax.rsqrt(mean_sq + RMS_EPS) * (1.0 + gains[pl.ds(which, 1), :])).astype(BF16)

    def norm(b, which):
        def body(i, _):
            norm_rows(b, which, block(i, NORM_ROWS))
            return 0

        lax.fori_loop(0, seq // NORM_ROWS, body, 0)

    def raw_copy(w, layer, c):
        rows = pl.ds(c * raw_rows, raw_rows)
        return pltpu.make_async_copy(w.at[layer, rows], raw.at[rows], raw_sem.at[c])

    def raw_start(w, layer):
        for c in range(n_raw):
            raw_copy(w, layer, c).start()

    def raw_wait(w, layer):
        for c in range(n_raw):
            raw_copy(w, layer, c).wait()

    def relayout(slot):
        for c in range(n_raw):
            rows = pl.ds(c * raw_rows, raw_rows)
            v = raw[rows].reshape(raw_rows, inner)
            wa[slot, rows, :] = v[:, :TILE]
            wb[slot, rows, :] = v[:, TILE:]

    def out_copy(layer, t):
        dst = (wa if t < 3 else wb).at[1, pl.ds((t % 3) * inner, inner), :]
        return pltpu.make_async_copy(w_out.at[layer, :, pl.ds(t * TILE, TILE)], dst, wo_sem.at[t])

    def gu_copies(layer, t, slot):
        c = block(t, TILE)
        return (
            pltpu.make_async_copy(w_gate.at[layer, :, c], wa.at[slot], wa_sem.at[slot]),
            pltpu.make_async_copy(w_up.at[layer, :, c], wb.at[slot], wb_sem.at[slot]),
        )

    def down_copies(layer, t, slot):
        c = block(t, TILE)
        return (
            pltpu.make_async_copy(w_down.at[layer, pl.ds(0, model), c], wa.at[slot], wa_sem.at[slot]),
            pltpu.make_async_copy(w_down.at[layer, pl.ds(model, model), c], wb.at[slot], wb_sem.at[slot]),
        )

    def start(copies):
        for c in copies:
            c.start()

    def wait(copies):
        for c in copies:
            c.wait()

    def dot(p, q):
        return jnp.dot(p, q, preferred_element_type=F32)

    def cache_copies(layer, b, h):
        return (
            pltpu.make_async_copy(m.at[:, block(heads + h, dim)], k_cache.at[layer, b, h], kc_sem.at[h]),
            pltpu.make_async_copy(m.at[:, block(h, dim)], v_cache.at[layer, b, h], vc_sem.at[h]),
        )

    def head(b, i, j):
        h = 2 * i + j
        lanes = slice(j * dim, (j + 1) * dim)
        cos_t, sin_t = cos_ref[...], sin_ref[...]

        def rope(v):
            lo, hi = v[:, :half_dim], v[:, half_dim:]
            return jnp.concatenate([lo * cos_t - hi * sin_t, hi * cos_t + lo * sin_t], axis=-1)

        q = (rope(ga[i, :, lanes]) * (dim ** -0.5)).astype(BF16)
        k = rope(ub[i, :, lanes]).astype(BF16)
        m[:, block(heads + h, dim)] = k
        for r in range(2):
            keys = (r + 1) * half
            v = m[pl.ds(0, keys), block(h, dim)]
            scores = lax.dot_general(q[r * half:keys], k[:keys], (((1,), (1,)), ((), ())), preferred_element_type=F32)
            row = r * half + lax.broadcasted_iota(jnp.int32, (half, keys), 0)
            col = lax.broadcasted_iota(jnp.int32, (half, keys), 1)
            scores = jnp.where((col <= row) & (col < len_ref[b]), scores, -1e30)
            p = jnp.exp(scores - jnp.max(scores, axis=-1, keepdims=True))
            p = (p * (1.0 / jnp.sum(p, axis=-1, keepdims=True))).astype(BF16)
            m[pl.ds(r * half, half), block(2 * heads + h, dim)] = dot(p, v).astype(BF16)

    hidden_copies = [pltpu.make_async_copy(hidden.at[b], x.at[b], x_sem.at[b]) for b in range(prompts)]

    def attn_phase(layer, b):
        @pl.when((layer == 0) & (b == 1))
        def _():
            hidden_copies[1].wait()

        @pl.when((layer == 0) | (b == 1))
        def _():
            norm(b, 2 * layer)

        raw_wait(w_query, layer)
        relayout(0)
        raw_start(w_key, layer)
        ga[0] = dot(a[...], wa[0])
        ga[1] = dot(a[...], wb[0])

        @pl.when(b == 1)
        def _():
            chip_add(0, 0, 2)
            chip_add(0, 0, 5)

        @pl.when((b == 0) & (layer > 0))
        def _():
            chip_add(1, 1, n_down - 1)

        raw_wait(w_key, layer)
        relayout(1)
        raw_start(w_value, layer)
        ub[0] = dot(a[...], wa[1])
        ub[1] = dot(a[...], wb[1])
        for t in range(n_down):
            out_copy(layer, t).start()
        raw_wait(w_value, layer)
        relayout(0)
        m[:, pl.ds(0, TILE)] = dot(a[...], wa[0]).astype(BF16)
        m[:, pl.ds(TILE, TILE)] = dot(a[...], wb[0]).astype(BF16)

        @pl.when(b == 0)
        def _():
            raw_start(w_query, layer)

        @pl.when(b == 1)
        def _():
            start(gu_copies(layer, 0, 0))

        def two_heads(i, _):
            head(b, i, 0)
            head(b, i, 1)
            start(cache_copies(layer, b, 2 * i))
            start(cache_copies(layer, b, 2 * i + 1))
            return 0

        lax.fori_loop(0, heads // 2, two_heads, 0)

        @pl.when((b == 0) & (layer > 0))
        def _():
            finish_sum(1, 1)

        for t in range(n_down):
            out_copy(layer, t).wait()
        o_cols = pl.ds(2 * inner, inner)

        def project(i, _):
            @pl.when(i > 0)
            def _():
                send_part(b, i - 1).start()
                send_part(b, i + 2).start()

            part[b, :, block(i, TILE)] = dot(m[:, o_cols], wa[1, block(i, inner), :]).astype(BF16)
            part[b, :, block(i + 3, TILE)] = dot(m[:, o_cols], wb[1, block(i, inner), :]).astype(BF16)
            return 0

        lax.fori_loop(0, 3, project, 0)
        for h in range(heads):
            wait(cache_copies(layer, b, h))
        send_part(b, 2).start()
        send_part(b, 5).start()
        for t in (0, 3, 1, 4):
            chip_add(b, 0, t)

        @pl.when((b == 0) & (layer > 0))
        def _():
            finish_wait(1, 1)

        @pl.when(b == 1)
        def _():
            chip_add(1, 0, 2)
            chip_add(1, 0, 5)
            finish_sum(0, 0)
            finish_wait(0, 0)

    def mlp_phase(layer, b):
        @pl.when((b == 1) & (layer + 1 < n_layers))
        def _():
            raw_start(w_query, layer + 1)

        @pl.when(b == 0)
        def _():
            norm(b, 2 * layer + 1)

        def gate_up(t, slot):
            wait(gu_copies(layer, t, slot))

            @pl.when(t + 1 < n_gu)
            def _():
                start(gu_copies(layer, t + 1, 1 - slot))

            @pl.when(t + 1 == n_gu)
            def _():
                start(down_copies(layer, 0, 1 - slot))

            gate = dot(a[...], wa[slot])
            up = dot(a[...], wb[slot])
            for r in range(0, seq, ACT_ROWS):
                act = jax.nn.gelu(gate[r:r + ACT_ROWS], approximate=True) * up[r:r + ACT_ROWS]
                m[pl.ds(r, ACT_ROWS), block(t, TILE)] = act.astype(BF16)

        def gate_up_pair(i, _):
            @pl.when(i == n_gu // 2 - 1)
            def _():
                finish_sum(1 - b, b)

            gate_up(2 * i, 0)

            @pl.when((i == 0) & (b == 1))
            def _():
                chip_add(0, 1, n_down - 1)

            gate_up(2 * i + 1, 1)
            return 0

        lax.fori_loop(0, n_gu // 2, gate_up_pair, 0)
        finish_wait(1 - b, b)
        next_norm = jnp.minimum(2 * layer + 1 + b, 2 * n_layers - 1)

        def down(t, slot):
            wait(down_copies(layer, t, slot))

            @pl.when(t + 1 < n_down)
            def _():
                start(down_copies(layer, t + 1, 1 - slot))

            @pl.when((t + 1 == n_down) & (b == 0))
            def _():
                start(gu_copies(layer, 0, 1 - slot))

            @pl.when(t > 0)
            def _():
                send_part(b, t - 1).start()

            @pl.when(t > 1)
            def _():
                chip_add(b, 1, t - 2)

            first = jnp.minimum(t * SPREAD_ROWS, seq - SPREAD_ROWS)
            for r in range(0, SPREAD_ROWS, ACT_ROWS):
                norm_rows(1 - b, next_norm, pl.ds(pl.multiple_of(first + r, ACT_ROWS), ACT_ROWS))
            part[b, :, block(t, TILE)] = (
                dot(m[:, pl.ds(0, model)], wa[slot]) + dot(m[:, pl.ds(model, model)], wb[slot])
            ).astype(BF16)

        def down_pair(i, _):
            down(2 * i, 0)
            down(2 * i + 1, 1)
            return 0

        lax.fori_loop(0, n_down // 2, down_pair, 0)
        send_part(b, n_down - 1).start()
        chip_add(b, 1, n_down - 2)

    hidden_copies[0].start()
    raw_start(w_query, 0)
    hidden_copies[1].start()
    barrier = pltpu.get_barrier_semaphore()
    for device in (peer, far):
        pl.semaphore_signal(barrier, inc=1, device_id=device, device_id_type=pl.DeviceIdType.MESH)
    hidden_copies[0].wait()
    pl.semaphore_wait(barrier, 2)

    def layer_step(layer, _):
        def attn_step(b, _):
            attn_phase(layer, b)
            return 0

        def mlp_step(b, _):
            mlp_phase(layer, b)
            return 0

        lax.fori_loop(0, prompts, attn_step, 0)
        lax.fori_loop(0, prompts, mlp_step, 0)
        return 0

    lax.fori_loop(0, n_layers, layer_step, 0)
    out_copies = [pltpu.make_async_copy(x.at[b], out, x_sem.at[b]) for b, out in enumerate((h_out0, h_out1))]
    out_copies[0].start()
    chip_add(1, 1, n_down - 1)
    finish_sum(1, 1)
    finish_wait(1, 1)
    out_copies[1].start()
    wait(out_copies)


def solution(mesh):
    head_cols = P(None, None, "tp", None)
    head_rows = P(None, "tp", None, None)
    ff_cols = P(None, None, "tp")
    ff_rows = P(None, "tp", None)

    def shard_body(hidden, lengths, w_query, w_key, w_value, w_out, w_gate, w_up, w_down, norm_attn, norm_mlp):
        n_layers, model, heads, dim = w_query.shape
        prompts, seq, _ = hidden.shape
        width = w_gate.shape[2]
        inner = heads * dim
        n_down = model // TILE
        half = seq // 2
        cos_t, sin_t = rope_tables(seq, dim)
        anywhere = pl.BlockSpec(memory_space=pl.ANY)
        vmem = pl.BlockSpec(memory_space=pltpu.VMEM)
        dma = pltpu.SemaphoreType.DMA
        cache = jax.ShapeDtypeStruct((n_layers, prompts, heads, seq, dim), BF16)
        gains = jnp.stack([norm_attn, norm_mlp], axis=1).reshape(2 * n_layers, model)
        state = jax.ShapeDtypeStruct(hidden.shape[1:], BF16)
        h0, h1, k_cache, v_cache = pl.pallas_call(
            kernel,
            in_specs=[pl.BlockSpec(memory_space=pltpu.SMEM)] + [anywhere] * 8 + [vmem] * 3,
            out_specs=[anywhere] * 4,
            out_shape=[state, state, cache, cache],
            scratch_shapes=[
                pltpu.VMEM((prompts, seq, model), BF16),
                pltpu.VMEM((seq, model), BF16),
                pltpu.VMEM((seq, width), BF16),
                pltpu.VMEM((2, model, TILE), BF16),
                pltpu.VMEM((2, model, TILE), BF16),
                pltpu.VMEM((model, heads, dim), BF16),
                pltpu.VMEM((2, seq, TILE), F32),
                pltpu.VMEM((2, seq, TILE), F32),
                pltpu.VMEM((prompts, seq, model), BF16),
                pltpu.VMEM((prompts, half, model), BF16),
                pltpu.VMEM((2, prompts, half, model), BF16),
                dma((prompts,)), dma((2,)), dma((2,)), dma((4,)), dma((n_down,)), dma((heads,)), dma((heads,)),
                dma((prompts, n_down)), dma((prompts, n_down)), dma((prompts, n_down)), dma((2, prompts, n_down)),
                dma((prompts, n_down)), dma((prompts, n_down)),
            ],
            compiler_params=pltpu.CompilerParams(
                collective_id=0, has_side_effects=True, vmem_limit_bytes=63 * 1024 * 1024
            ),
        )(
            lengths, hidden, w_query, w_key, w_value, w_out.reshape(n_layers, inner, model), w_gate, w_up, w_down,
            gains, cos_t, sin_t,
        )
        return jnp.stack([h0, h1]), k_cache, v_cache

    return jax.shard_map(
        shard_body,
        mesh=mesh,
        in_specs=(P("dp"), P("dp"), head_cols, head_cols, head_cols, head_rows, ff_cols, ff_cols, ff_rows, P(), P()),
        out_specs=(P("dp"), P(None, "dp", "tp"), P(None, "dp", "tp")),
        check_vma=False,
    )
```

```python
import jax
import jax.numpy as jnp
import numpy as np
from jax import lax
from jax.experimental import pallas as pl
from jax.experimental.pallas import tpu as pltpu
from jax.sharding import PartitionSpec as P

RMS_EPS = 1e-6
ROPE_BASE = 10000.0
TILE = 512
NORM_ROWS = 64
ACT_ROWS = 16
SPREAD_ROWS = 176
F32, BF16 = jnp.float32, jnp.bfloat16


def rope_tables(seq_len, head_dim):
    half_dim = head_dim // 2
    inv_freq = np.float32(ROPE_BASE) ** (-np.arange(half_dim, dtype=np.float32) * np.float32(2.0 / head_dim))
    angles = np.arange(seq_len, dtype=np.float32)[:, None] * inv_freq[None, :].astype(np.float32)
    return np.cos(angles).astype(np.float32), np.sin(angles).astype(np.float32)


def block(i, size):
    return pl.ds(pl.multiple_of(i * size, size), size)


def kernel(
    len_ref, hidden, w_query, w_key, w_value, w_out, w_gate, w_up, w_down, gains, cos_ref, sin_ref,
    h_out0, h_out1, k_cache, v_cache,
    x, a, m, wa, wb, raw, ga, ub, part, recv1, recv2,
    x_sem, wa_sem, wb_sem, raw_sem, wo_sem, kc_sem, vc_sem, s1, r1, s2, r2, s3, r3,
):
    n_layers, model, heads, dim = w_query.shape
    prompts, seq, _ = hidden.shape
    inner = heads * dim
    n_gu = w_gate.shape[2] // TILE
    n_down = model // TILE
    half = seq // 2
    n_raw = raw_sem.shape[0]
    raw_rows = model // n_raw
    half_dim = dim // 2

    me = lax.axis_index("tp")
    core = lax.rem(me, 2)
    peer = {"tp": me + 1 - 2 * core}
    far = {"tp": lax.rem(me + 2, 4)}
    own_row = core * half
    other_row = (1 - core) * half

    def rows_from(start, size):
        return pl.ds(pl.multiple_of(start, 128), size)

    def piece(stage, t):
        if stage == 0:
            j = lax.div(jnp.int32(t), 3)
            return j * (half // 2), half // 2, block(t - 3 * j, 2 * TILE)
        return 0, half, block(t, TILE)

    def remote(src, dst, send_sem, recv_sem, device):
        return pltpu.make_async_remote_copy(src, dst, send_sem, recv_sem, device_id=device, device_id_type=pl.DeviceIdType.MESH)

    def send_part(b, stage, t):
        row, n, c = piece(stage, t)
        return remote(
            part.at[b, rows_from(other_row + row, n), c], recv1.at[b, rows_from(row, n), c], s1.at[b, t], r1.at[b, t], peer
        )

    def send_far(b, stage, t):
        row, n, c = piece(stage, t)
        return remote(
            part.at[b, rows_from(own_row + row, n), c], recv2.at[stage, b, rows_from(row, n), c],
            s2.at[b, t], r2.at[stage, b, t], far,
        )

    def send_x(b, stage, t):
        row, n, c = piece(stage, t)
        rows = rows_from(own_row + row, n)
        return remote(x.at[b, rows, c], x.at[b, rows, c], s3.at[b, t], r3.at[b, t], peer)

    def chip_add(b, stage, t):
        row, n, c = piece(stage, t)
        rows = rows_from(own_row + row, n)
        send_part(b, stage, t).wait_recv()
        part[b, rows, c] = (part[b, rows, c].astype(F32) + recv1[b, rows_from(row, n), c].astype(F32)).astype(BF16)
        send_far(b, stage, t).start()

    def chip_adds(b, stage, first, last):
        def body(t, _):
            chip_add(b, stage, t)
            return 0

        lax.fori_loop(first, last, body, 0)

    def finish_sum(b, stage, first, last):
        def body(t, _):
            row, n, c = piece(stage, t)
            rows = rows_from(own_row + row, n)
            send_far(b, stage, t).wait_recv()
            total = part[b, rows, c].astype(F32) + recv2[stage, b, rows_from(row, n), c].astype(F32)
            x[b, rows, c] = (x[b, rows, c].astype(F32) + total).astype(BF16)
            send_x(b, stage, t).start()
            return 0

        lax.fori_loop(first, last, body, 0)

    def finish_wait(b, stage, first, last):
        def body(t, _):
            send_part(b, stage, t).wait_send()
            send_far(b, stage, t).wait_send()
            send_x(b, stage, t).wait()
            return 0

        lax.fori_loop(first, last, body, 0)

    def norm_rows(b, which, rows):
        v = x[b, rows, :].astype(F32)
        mean_sq = jnp.mean(v * v, axis=-1, keepdims=True)
        a[rows, :] = (v * lax.rsqrt(mean_sq + RMS_EPS) * (1.0 + gains[pl.ds(which, 1), :])).astype(BF16)

    def norm(b, which):
        def body(i, _):
            norm_rows(b, which, block(i, NORM_ROWS))
            return 0

        lax.fori_loop(0, seq // NORM_ROWS, body, 0)

    def raw_copy(w, layer, c):
        rows = pl.ds(c * raw_rows, raw_rows)
        return pltpu.make_async_copy(w.at[layer, rows], raw.at[rows], raw_sem.at[c])

    def raw_start(w, layer):
        for c in range(n_raw):
            raw_copy(w, layer, c).start()

    def relayout(slot, w, layer, then=None):
        for c in range(n_raw):
            raw_copy(w, layer, c).wait()
        for c in range(n_raw):
            rows = pl.ds(c * raw_rows, raw_rows)
            v = raw[rows].reshape(raw_rows, inner)
            wa[slot, rows, :] = v[:, :TILE]
            wb[slot, rows, :] = v[:, TILE:]
            if then is not None:
                raw_copy(then, layer, c).start()

    def out_copy(layer, t):
        dst = (wb if t % 2 else wa).at[1, pl.ds((t // 2) * inner, inner), :]
        return pltpu.make_async_copy(w_out.at[layer, :, pl.ds(t * TILE, TILE)], dst, wo_sem.at[t])

    def gu_copies(layer, t, slot):
        c = block(t, TILE)
        return (
            pltpu.make_async_copy(w_gate.at[layer, :, c], wa.at[slot], wa_sem.at[slot]),
            pltpu.make_async_copy(w_up.at[layer, :, c], wb.at[slot], wb_sem.at[slot]),
        )

    def down_copies(layer, t, slot):
        c = block(t, TILE)
        return (
            pltpu.make_async_copy(w_down.at[layer, pl.ds(0, model), c], wa.at[slot], wa_sem.at[slot]),
            pltpu.make_async_copy(w_down.at[layer, pl.ds(model, model), c], wb.at[slot], wb_sem.at[slot]),
        )

    def start(copies):
        for c in copies:
            c.start()

    def wait(copies):
        for c in copies:
            c.wait()

    def dot(p, q):
        return jnp.dot(p, q, preferred_element_type=F32)

    def cache_copies(layer, b, h):
        return (
            pltpu.make_async_copy(m.at[:, block(heads + h, dim)], k_cache.at[layer, b, h], kc_sem.at[h]),
            pltpu.make_async_copy(m.at[:, block(h, dim)], v_cache.at[layer, b, h], vc_sem.at[h]),
        )

    def head(b, i, j):
        h = 2 * i + j
        lanes = slice(j * dim, (j + 1) * dim)
        cos_t, sin_t = cos_ref[...], sin_ref[...]

        def rope(v):
            lo, hi = v[:, :half_dim], v[:, half_dim:]
            return jnp.concatenate([lo * cos_t - hi * sin_t, hi * cos_t + lo * sin_t], axis=-1)

        q = (rope(ga[i, :, lanes]) * (dim ** -0.5)).astype(BF16)
        k = rope(ub[i, :, lanes]).astype(BF16)
        m[:, block(heads + h, dim)] = k
        for r in range(2):
            keys = (r + 1) * half
            v = m[pl.ds(0, keys), block(h, dim)]
            scores = lax.dot_general(q[r * half:keys], k[:keys], (((1,), (1,)), ((), ())), preferred_element_type=F32)
            row = r * half + lax.broadcasted_iota(jnp.int32, (half, keys), 0)
            col = lax.broadcasted_iota(jnp.int32, (half, keys), 1)
            scores = jnp.where((col <= row) & (col < len_ref[b]), scores, -1e30)
            p = jnp.exp(scores - jnp.max(scores, axis=-1, keepdims=True))
            p = (p * (1.0 / jnp.sum(p, axis=-1, keepdims=True))).astype(BF16)
            m[pl.ds(r * half, half), block(2 * heads + h, dim)] = dot(p, v).astype(BF16)

    hidden_copies = [pltpu.make_async_copy(hidden.at[b], x.at[b], x_sem.at[b]) for b in range(prompts)]

    def attn_phase(layer, b):
        @pl.when((layer == 0) & (b == 1))
        def _():
            hidden_copies[1].wait()

        @pl.when((layer == 0) | (b == 1))
        def _():
            norm(b, 2 * layer)

        @pl.when(b == 1)
        def _():
            chip_adds(0, 0, 2, n_down)

        relayout(0, w_query, layer, w_key)
        ga[0] = dot(a[...], wa[0])
        ga[1] = dot(a[...], wb[0])

        @pl.when((b == 0) & (layer > 0))
        def _():
            chip_add(1, 1, n_down - 1)

        relayout(1, w_key, layer, w_value)
        ub[0] = dot(a[...], wa[1])
        ub[1] = dot(a[...], wb[1])
        for t in range(n_down):
            out_copy(layer, t).start()
        relayout(0, w_value, layer)
        m[:, pl.ds(0, TILE)] = dot(a[...], wa[0]).astype(BF16)
        m[:, pl.ds(TILE, TILE)] = dot(a[...], wb[0]).astype(BF16)

        @pl.when(b == 0)
        def _():
            raw_start(w_query, layer)

        @pl.when(b == 1)
        def _():
            start(gu_copies(layer, 0, 0))

        def two_heads(i, _):
            head(b, i, 0)
            head(b, i, 1)
            start(cache_copies(layer, b, 2 * i))
            start(cache_copies(layer, b, 2 * i + 1))
            return 0

        lax.fori_loop(0, heads // 2, two_heads, 0)

        @pl.when((b == 0) & (layer > 0))
        def _():
            finish_sum(1, 1, 0, n_down)

        for t in range(n_down):
            out_copy(layer, t).wait()
        o_cols = pl.ds(2 * inner, inner)

        def send_both(i):
            send_part(b, 0, i).start()
            send_part(b, 0, i + 3).start()

        def project(i, _):
            @pl.when(i > 0)
            def _():
                send_both(i - 1)

            part[b, :, block(2 * i, TILE)] = dot(m[:, o_cols], wa[1, block(i, inner), :]).astype(BF16)
            part[b, :, block(2 * i + 1, TILE)] = dot(m[:, o_cols], wb[1, block(i, inner), :]).astype(BF16)
            return 0

        lax.fori_loop(0, 3, project, 0)
        for h in range(heads):
            wait(cache_copies(layer, b, h))
        send_both(2)
        chip_adds(b, 0, 0, 2)

        @pl.when((b == 0) & (layer > 0))
        def _():
            finish_wait(1, 1, 0, n_down)

    def mlp_phase(layer, b):
        @pl.when((b == 1) & (layer + 1 < n_layers))
        def _():
            raw_start(w_query, layer + 1)

        def gate_up(t, after, slot, h):
            wait(gu_copies(layer, t, slot))

            @pl.when(after < n_gu)
            def _():
                start(gu_copies(layer, after, 1 - slot))

            @pl.when(after == n_gu)
            def _():
                start(down_copies(layer, 0, 1 - slot))

            if h is None:
                lhs = a[...]
                starts = range(0, seq, ACT_ROWS)
            else:
                quarter = half // 2
                lows = [rows_from(i * half + h * quarter, quarter) for i in range(2)]
                lhs = jnp.concatenate([a[r, :] for r in lows], axis=0)
                starts = [i * half + h * quarter + r for i in range(2) for r in range(0, quarter, ACT_ROWS)]
            gate = dot(lhs, wa[slot])
            up = dot(lhs, wb[slot])
            for i, row in enumerate(starts):
                r = i * ACT_ROWS
                act = jax.nn.gelu(gate[r:r + ACT_ROWS], approximate=True) * up[r:r + ACT_ROWS]
                m[pl.ds(row if h is None else pl.multiple_of(row, ACT_ROWS), ACT_ROWS), block(t, TILE)] = act.astype(BF16)

        def norm_half(h):
            def body(i, _):
                j = lax.div(i, 2)
                norm_rows(0, 2 * layer + 1, pl.ds(pl.multiple_of(j * half + h * (half // 2) + (i - 2 * j) * NORM_ROWS, NORM_ROWS), NORM_ROWS))
                return 0

            lax.fori_loop(0, 4, body, 0)

        @pl.when(b == 0)
        def _():
            finish_sum(0, 0, 0, 3)
            chip_adds(1, 0, 2, n_down)
            finish_wait(0, 0, 0, 3)
            norm_half(0)

            def step(u, _):
                h = lax.div(u, n_gu)

                @pl.when(u == n_gu - 1)
                def _():
                    finish_sum(0, 0, 3, n_down)

                @pl.when(u == n_gu)
                def _():
                    finish_wait(0, 0, 3, n_down)
                    norm_half(1)

                t = u - h * n_gu
                last = u == 2 * n_gu - 1
                after = jnp.where(last, n_gu, lax.rem(u + 1, n_gu))
                gate_up(t, after, lax.rem(u, 2), h)
                return 0

            lax.fori_loop(0, 2 * n_gu, step, 0)

        @pl.when(b == 1)
        def _():
            def step(t, _):
                @pl.when(t == 1)
                def _():
                    chip_add(0, 1, n_down - 1)

                gate_up(t, t + 1, lax.rem(t, 2), None)
                return 0

            lax.fori_loop(0, n_gu, step, 0)

        next_norm = jnp.minimum(2 * layer + 1 + b, 2 * n_layers - 1)

        def down(t, with_norm):
            slot = lax.rem(t, 2)
            wait(down_copies(layer, t, slot))

            @pl.when(t + 1 < n_down)
            def _():
                start(down_copies(layer, t + 1, 1 - slot))

            @pl.when((t + 1 == n_down) & (b == 0))
            def _():
                start(gu_copies(layer, 0, 1 - slot))

            @pl.when(t > 0)
            def _():
                send_part(b, 1, t - 1).start()

            @pl.when(t > 1)
            def _():
                chip_add(b, 1, t - 2)

            if with_norm:
                first = jnp.minimum((t - 3) * SPREAD_ROWS, seq - SPREAD_ROWS)
                for r in range(0, SPREAD_ROWS, ACT_ROWS):
                    norm_rows(1 - b, next_norm, pl.ds(pl.multiple_of(first + r, ACT_ROWS), ACT_ROWS))
            part[b, :, block(t, TILE)] = (
                dot(m[:, pl.ds(0, model)], wa[slot]) + dot(m[:, pl.ds(model, model)], wb[slot])
            ).astype(BF16)

        def down_plain(t, _):
            @pl.when((t == 2) & (b == 0))
            def _():
                finish_sum(1, 0, 0, n_down)

            @pl.when((t == 2) & (b == 1))
            def _():
                finish_sum(0, 1, 0, n_down)

            down(t, False)
            return 0

        def down_norm(t, _):
            down(t, True)
            return 0

        lax.fori_loop(0, 3, down_plain, 0)

        @pl.when(b == 0)
        def _():
            finish_wait(1, 0, 0, n_down)

        @pl.when(b == 1)
        def _():
            finish_wait(0, 1, 0, n_down)

        lax.fori_loop(3, n_down, down_norm, 0)
        send_part(b, 1, n_down - 1).start()
        chip_add(b, 1, n_down - 2)

    hidden_copies[0].start()
    raw_start(w_query, 0)
    hidden_copies[1].start()
    barrier = pltpu.get_barrier_semaphore()
    for device in (peer, far):
        pl.semaphore_signal(barrier, inc=1, device_id=device, device_id_type=pl.DeviceIdType.MESH)
    hidden_copies[0].wait()
    pl.semaphore_wait(barrier, 2)

    def layer_step(layer, _):
        def attn_step(b, _):
            attn_phase(layer, b)
            return 0

        def mlp_step(b, _):
            mlp_phase(layer, b)
            return 0

        lax.fori_loop(0, prompts, attn_step, 0)
        lax.fori_loop(0, prompts, mlp_step, 0)
        return 0

    lax.fori_loop(0, n_layers, layer_step, 0)
    out_copies = [pltpu.make_async_copy(x.at[b], out, x_sem.at[b]) for b, out in enumerate((h_out0, h_out1))]
    out_copies[0].start()
    chip_add(1, 1, n_down - 1)
    finish_sum(1, 1, 0, n_down)
    finish_wait(1, 1, 0, n_down)
    out_copies[1].start()
    wait(out_copies)


def solution(mesh):
    head_cols = P(None, None, "tp", None)
    head_rows = P(None, "tp", None, None)
    ff_cols = P(None, None, "tp")
    ff_rows = P(None, "tp", None)

    def shard_body(hidden, lengths, w_query, w_key, w_value, w_out, w_gate, w_up, w_down, norm_attn, norm_mlp):
        n_layers, model, heads, dim = w_query.shape
        prompts, seq, _ = hidden.shape
        width = w_gate.shape[2]
        inner = heads * dim
        n_down = model // TILE
        half = seq // 2
        cos_t, sin_t = rope_tables(seq, dim)
        anywhere = pl.BlockSpec(memory_space=pl.ANY)
        vmem = pl.BlockSpec(memory_space=pltpu.VMEM)
        dma = pltpu.SemaphoreType.DMA
        cache = jax.ShapeDtypeStruct((n_layers, prompts, heads, seq, dim), BF16)
        gains = jnp.stack([norm_attn, norm_mlp], axis=1).reshape(2 * n_layers, model)
        state = jax.ShapeDtypeStruct(hidden.shape[1:], BF16)
        h0, h1, k_cache, v_cache = pl.pallas_call(
            kernel,
            in_specs=[pl.BlockSpec(memory_space=pltpu.SMEM)] + [anywhere] * 8 + [vmem] * 3,
            out_specs=[anywhere] * 4,
            out_shape=[state, state, cache, cache],
            scratch_shapes=[
                pltpu.VMEM((prompts, seq, model), BF16),
                pltpu.VMEM((seq, model), BF16),
                pltpu.VMEM((seq, width), BF16),
                pltpu.VMEM((2, model, TILE), BF16),
                pltpu.VMEM((2, model, TILE), BF16),
                pltpu.VMEM((model, heads, dim), BF16),
                pltpu.VMEM((2, seq, TILE), F32),
                pltpu.VMEM((2, seq, TILE), F32),
                pltpu.VMEM((prompts, seq, model), BF16),
                pltpu.VMEM((prompts, half, model), BF16),
                pltpu.VMEM((2, prompts, half, model), BF16),
                dma((prompts,)), dma((2,)), dma((2,)), dma((4,)), dma((n_down,)), dma((heads,)), dma((heads,)),
                dma((prompts, n_down)), dma((prompts, n_down)), dma((prompts, n_down)), dma((2, prompts, n_down)),
                dma((prompts, n_down)), dma((prompts, n_down)),
            ],
            compiler_params=pltpu.CompilerParams(
                collective_id=0, has_side_effects=True, vmem_limit_bytes=63 * 1024 * 1024
            ),
        )(
            lengths, hidden, w_query, w_key, w_value, w_out.reshape(n_layers, inner, model), w_gate, w_up, w_down,
            gains, cos_t, sin_t,
        )
        return jnp.stack([h0, h1]), k_cache, v_cache

    return jax.shard_map(
        shard_body,
        mesh=mesh,
        in_specs=(P("dp"), P("dp"), head_cols, head_cols, head_cols, head_rows, ff_cols, ff_cols, ff_rows, P(), P()),
        out_specs=(P("dp"), P(None, "dp", "tp"), P(None, "dp", "tp")),
        check_vma=False,
    )
```

```python
import jax
import jax.numpy as jnp
import numpy as np
from jax import lax
from jax.experimental import pallas as pl
from jax.experimental.pallas import tpu as pltpu
from jax.sharding import PartitionSpec as P

RMS_EPS = 1e-6
ROPE_BASE = 10000.0
TILE = 512
SLOTS = 3
NORM_ROWS = 64
ACT_ROWS = 16
SPREAD_ROWS = 176
F32, BF16 = jnp.float32, jnp.bfloat16


def rope_tables(seq_len, head_dim):
    half_dim = head_dim // 2
    inv_freq = np.float32(ROPE_BASE) ** (-np.arange(half_dim, dtype=np.float32) * np.float32(2.0 / head_dim))
    angles = np.arange(seq_len, dtype=np.float32)[:, None] * inv_freq[None, :].astype(np.float32)
    return np.cos(angles).astype(np.float32), np.sin(angles).astype(np.float32)


def block(i, size):
    return pl.ds(pl.multiple_of(i * size, size), size)


def kernel(
    len_ref, hidden, w_query, w_key, w_value, w_out, w_gate, w_up, w_down, gain_attn, gain_mlp, cos_ref, sin_ref,
    h_out0, h_out1, k_cache, v_cache,
    x, a, m, wa, wb, raw, part, recv1, recv2, gains,
    x_sem, wa_sem, wb_sem, raw_sem, wo_sem, kc_sem, vc_sem, s1, r1, s2, r2, s3, r3, credit,
):
    n_layers, model, heads, dim = w_query.shape
    prompts, seq, _ = hidden.shape
    inner = heads * dim
    n_gu = w_gate.shape[2] // TILE
    n_down = model // TILE
    half = seq // 2
    n_raw = raw_sem.shape[0]
    raw_rows = model // n_raw
    half_dim = dim // 2

    me = lax.axis_index("tp")
    core = lax.rem(me, 2)
    peer = {"tp": me + 1 - 2 * core}
    far = {"tp": lax.rem(me + 2, 4)}
    own_row = core * half
    other_row = (1 - core) * half

    def rows_from(start, size):
        return pl.ds(pl.multiple_of(start, 128), size)

    def piece(stage, t):
        if stage == 0:
            j = lax.div(jnp.int32(t), 3)
            return j * (half // 2), half // 2, block(t - 3 * j, 2 * TILE)
        return 0, half, block(t, TILE)

    def remote(src, dst, send_sem, recv_sem, device):
        return pltpu.make_async_remote_copy(src, dst, send_sem, recv_sem, device_id=device, device_id_type=pl.DeviceIdType.MESH)

    def send_part(b, stage, t):
        row, n, c = piece(stage, t)
        return remote(
            part.at[b, rows_from(other_row + row, n), c], recv1.at[b, rows_from(row, n), c], s1.at[b, t], r1.at[b, t], peer
        )

    def send_far(b, stage, t):
        row, n, c = piece(stage, t)
        return remote(
            part.at[b, rows_from(own_row + row, n), c], recv2.at[b, rows_from(row, n), c],
            s2.at[b, t], r2.at[b, t], far,
        )

    def send_x(b, stage, t):
        row, n, c = piece(stage, t)
        rows = rows_from(own_row + row, n)
        return remote(x.at[b, rows, c], x.at[b, rows, c], s3.at[b, t], r3.at[b, t], peer)

    def chip_add(b, stage, t):
        row, n, c = piece(stage, t)
        rows = rows_from(own_row + row, n)
        send_part(b, stage, t).wait_recv()
        part[b, rows, c] = (part[b, rows, c].astype(F32) + recv1[b, rows_from(row, n), c].astype(F32)).astype(BF16)
        send_far(b, stage, t).start()

    def chip_adds(b, stage, first, last):
        def body(t, _):
            chip_add(b, stage, t)
            return 0

        lax.fori_loop(first, last, body, 0)

    def finish_sum(b, stage, first, last):
        def body(t, _):
            row, n, c = piece(stage, t)
            rows = rows_from(own_row + row, n)
            send_far(b, stage, t).wait_recv()
            total = part[b, rows, c].astype(F32) + recv2[b, rows_from(row, n), c].astype(F32)
            x[b, rows, c] = (x[b, rows, c].astype(F32) + total).astype(BF16)
            send_x(b, stage, t).start()
            return 0

        lax.fori_loop(first, last, body, 0)
        if last == n_down:
            pl.semaphore_signal(credit.at[b], inc=1, device_id=far, device_id_type=pl.DeviceIdType.MESH)

    def finish_wait(b, stage, first, last):
        def body(t, _):
            send_part(b, stage, t).wait_send()
            send_far(b, stage, t).wait_send()
            send_x(b, stage, t).wait()
            return 0

        lax.fori_loop(first, last, body, 0)

    def norm_rows(b, which, rows):
        v = x[b, rows, :].astype(F32)
        mean_sq = jnp.mean(v * v, axis=-1, keepdims=True)
        a[rows, :] = (v * lax.rsqrt(mean_sq + RMS_EPS) * (1.0 + gains[pl.ds(which, 1), :])).astype(BF16)

    def norm(b, which):
        def body(i, _):
            norm_rows(b, which, block(i, NORM_ROWS))
            return 0

        lax.fori_loop(0, seq // NORM_ROWS, body, 0)

    def raw_copy(w, layer, c):
        rows = pl.ds(c * raw_rows, raw_rows)
        return pltpu.make_async_copy(w.at[layer, rows], raw.at[rows], raw_sem.at[c])

    def raw_start(w, layer):
        for c in range(n_raw):
            raw_copy(w, layer, c).start()

    def relayout(slot, w, layer, then=None):
        for c in range(n_raw):
            raw_copy(w, layer, c).wait()
        for c in range(n_raw):
            rows = pl.ds(c * raw_rows, raw_rows)
            v = raw[rows].reshape(raw_rows, inner)
            wa[slot, rows, :] = v[:, :TILE]
            wb[slot, rows, :] = v[:, TILE:]
            if then is not None:
                raw_copy(then, layer, c).start()

    def out_copy(layer, t):
        dst = (wb if t % 2 else wa).at[2, pl.ds((t // 2) * inner, inner), :]
        return pltpu.make_async_copy(w_out.at[layer, :, pl.ds(t * TILE, TILE)], dst, wo_sem.at[t])

    def gu_copies(layer, t, slot):
        c = block(t, TILE)
        return (
            pltpu.make_async_copy(w_gate.at[layer, :, c], wa.at[slot], wa_sem.at[slot]),
            pltpu.make_async_copy(w_up.at[layer, :, c], wb.at[slot], wb_sem.at[slot]),
        )

    def down_copies(layer, t, slot):
        c = block(t, TILE)
        return (
            pltpu.make_async_copy(w_down.at[layer, pl.ds(0, model), c], wa.at[slot], wa_sem.at[slot]),
            pltpu.make_async_copy(w_down.at[layer, pl.ds(model, model), c], wb.at[slot], wb_sem.at[slot]),
        )

    def start(copies):
        for c in copies:
            c.start()

    def wait(copies):
        for c in copies:
            c.wait()

    def dot(p, q):
        return jnp.dot(p, q, preferred_element_type=F32)

    def cache_copies(layer, b, h):
        return (
            pltpu.make_async_copy(m.at[:, block(heads + h, dim)], k_cache.at[layer, b, h], kc_sem.at[h]),
            pltpu.make_async_copy(m.at[:, block(h, dim)], v_cache.at[layer, b, h], vc_sem.at[h]),
        )

    def rotate(v, first, scale):
        for r in range(0, seq, ACT_ROWS):
            rows = pl.ds(r, ACT_ROWS)
            cos_t, sin_t = cos_ref[rows, :], sin_ref[rows, :]
            for c in range(0, TILE, dim):
                lo, hi = v[r:r + ACT_ROWS, c:c + half_dim], v[r:r + ACT_ROWS, c + half_dim:c + dim]
                for d, w in ((0, lo * cos_t - hi * sin_t), (half_dim, hi * cos_t + lo * sin_t)):
                    w = w if scale is None else w * scale
                    m[rows, pl.ds(first + c + d, half_dim)] = w.astype(BF16)

    def head(b, i, j):
        h = 2 * i + j
        q = m[:, block(3 * heads + h, dim)]
        k = m[:, block(heads + h, dim)]
        for r in range(2):
            keys = (r + 1) * half
            v = m[pl.ds(0, keys), block(h, dim)]
            scores = lax.dot_general(q[r * half:keys], k[:keys], (((1,), (1,)), ((), ())), preferred_element_type=F32)
            row = r * half + lax.broadcasted_iota(jnp.int32, (half, keys), 0)
            col = lax.broadcasted_iota(jnp.int32, (half, keys), 1)
            scores = jnp.where((col <= row) & (col < len_ref[b]), scores, -1e30)
            p = jnp.exp(scores - jnp.max(scores, axis=-1, keepdims=True))
            p = (p * (1.0 / jnp.sum(p, axis=-1, keepdims=True))).astype(BF16)
            m[pl.ds(r * half, half), block(2 * heads + h, dim)] = dot(p, v).astype(BF16)

    hidden_copies = [pltpu.make_async_copy(hidden.at[b], x.at[b], x_sem.at[b]) for b in range(prompts)]

    def attn_phase(layer, b):
        @pl.when((layer == 0) & (b == 1))
        def _():
            hidden_copies[1].wait()

        @pl.when((layer == 0) | (b == 1))
        def _():
            norm(b, 2 * layer)

        @pl.when(b == 1)
        def _():
            chip_adds(0, 0, 2, n_down)

        relayout(0, w_query, layer, w_key)
        rotate(dot(a[...], wa[0]), 3 * inner, dim ** -0.5)
        rotate(dot(a[...], wb[0]), 3 * inner + TILE, dim ** -0.5)

        @pl.when((b == 0) & (layer > 0))
        def _():
            chip_add(1, 1, n_down - 1)

        relayout(1, w_key, layer, w_value)
        rotate(dot(a[...], wa[1]), inner, None)
        rotate(dot(a[...], wb[1]), inner + TILE, None)
        for t in range(n_down):
            out_copy(layer, t).start()
        relayout(0, w_value, layer)
        m[:, pl.ds(0, TILE)] = dot(a[...], wa[0]).astype(BF16)
        m[:, pl.ds(TILE, TILE)] = dot(a[...], wb[0]).astype(BF16)

        @pl.when(b == 0)
        def _():
            raw_start(w_query, layer)

        @pl.when(b == 1)
        def _():
            start(gu_copies(layer, 0, 0))
            start(gu_copies(layer, 1, 1))

        def two_heads(i, _):
            head(b, i, 0)
            head(b, i, 1)
            start(cache_copies(layer, b, 2 * i))
            start(cache_copies(layer, b, 2 * i + 1))
            return 0

        lax.fori_loop(0, heads // 2, two_heads, 0)

        @pl.when((b == 0) & (layer > 0))
        def _():
            finish_sum(1, 1, 0, n_down)

        for t in range(n_down):
            out_copy(layer, t).wait()
        o_cols = pl.ds(2 * inner, inner)

        def send_both(i):
            send_part(b, 0, i).start()
            send_part(b, 0, i + 3).start()

        def project(i, _):
            @pl.when(i > 0)
            def _():
                send_both(i - 1)

            part[b, :, block(2 * i, TILE)] = dot(m[:, o_cols], wa[2, block(i, inner), :]).astype(BF16)
            part[b, :, block(2 * i + 1, TILE)] = dot(m[:, o_cols], wb[2, block(i, inner), :]).astype(BF16)
            return 0

        lax.fori_loop(0, 3, project, 0)
        for h in range(heads):
            wait(cache_copies(layer, b, h))
        send_both(2)

        @pl.when(layer > 0)
        def _():
            pl.semaphore_wait(credit.at[b], 1)

        chip_adds(b, 0, 0, 2)

        @pl.when((b == 0) & (layer > 0))
        def _():
            finish_wait(1, 1, 0, n_down)

    def mlp_phase(layer, b):
        @pl.when((b == 1) & (layer + 1 < n_layers))
        def _():
            raw_start(w_query, layer + 1)

        def gate_up(u, steps, h):
            slot, ahead = lax.rem(u, SLOTS), u + 2
            slot_ahead = lax.rem(ahead, SLOTS)
            t = lax.rem(u, n_gu)
            wait(gu_copies(layer, t, slot))

            @pl.when(ahead < steps)
            def _():
                start(gu_copies(layer, lax.rem(ahead, n_gu), slot_ahead))

            @pl.when(ahead >= steps)
            def _():
                start(down_copies(layer, ahead - steps, slot_ahead))

            if h is None:
                lhs = a[...]
                starts = range(0, seq, ACT_ROWS)
            else:
                quarter = half // 2
                lows = [rows_from(i * half + h * quarter, quarter) for i in range(2)]
                lhs = jnp.concatenate([a[r, :] for r in lows], axis=0)
                starts = [i * half + h * quarter + r for i in range(2) for r in range(0, quarter, ACT_ROWS)]
            gate = dot(lhs, wa[slot])
            up = dot(lhs, wb[slot])
            for i, row in enumerate(starts):
                r = i * ACT_ROWS
                act = jax.nn.gelu(gate[r:r + ACT_ROWS], approximate=True) * up[r:r + ACT_ROWS]
                m[pl.ds(row if h is None else pl.multiple_of(row, ACT_ROWS), ACT_ROWS), block(t, TILE)] = act.astype(BF16)

        def norm_half(h):
            def body(i, _):
                j = lax.div(i, 2)
                norm_rows(0, 2 * layer + 1, pl.ds(pl.multiple_of(j * half + h * (half // 2) + (i - 2 * j) * NORM_ROWS, NORM_ROWS), NORM_ROWS))
                return 0

            lax.fori_loop(0, 4, body, 0)

        @pl.when(b == 0)
        def _():
            finish_sum(0, 0, 0, 3)
            chip_adds(1, 0, 2, n_down)
            finish_wait(0, 0, 0, 3)
            norm_half(0)

            def step(u, _):
                h = lax.div(u, n_gu)

                @pl.when(u == n_gu - 1)
                def _():
                    finish_sum(0, 0, 3, n_down)

                @pl.when(u == n_gu)
                def _():
                    finish_wait(0, 0, 3, n_down)
                    norm_half(1)

                gate_up(u, 2 * n_gu, h)
                return 0

            lax.fori_loop(0, 2 * n_gu, step, 0)

        @pl.when(b == 1)
        def _():
            def step(t, _):
                @pl.when(t == 1)
                def _():
                    chip_add(0, 1, n_down - 1)

                gate_up(t, n_gu, None)
                return 0

            lax.fori_loop(0, n_gu, step, 0)

        next_norm = jnp.minimum(2 * layer + 1 + b, 2 * n_layers - 1)

        def down(t, with_norm):
            slot, ahead = lax.rem(t, SLOTS), t + 2
            slot_ahead = lax.rem(ahead, SLOTS)
            wait(down_copies(layer, t, slot))

            @pl.when(ahead < n_down)
            def _():
                start(down_copies(layer, ahead, slot_ahead))

            @pl.when((ahead >= n_down) & (b == 0))
            def _():
                start(gu_copies(layer, ahead - n_down, slot_ahead))

            @pl.when(t > 0)
            def _():
                send_part(b, 1, t - 1).start()

            @pl.when(t == 2)
            def _():
                pl.semaphore_wait(credit.at[b], 1)

            @pl.when(t > 1)
            def _():
                chip_add(b, 1, t - 2)

            if with_norm:
                first = jnp.minimum((t - 3) * SPREAD_ROWS, seq - SPREAD_ROWS)
                for r in range(0, SPREAD_ROWS, ACT_ROWS):
                    norm_rows(1 - b, next_norm, pl.ds(pl.multiple_of(first + r, ACT_ROWS), ACT_ROWS))
            part[b, :, block(t, TILE)] = (
                dot(m[:, pl.ds(0, model)], wa[slot]) + dot(m[:, pl.ds(model, model)], wb[slot])
            ).astype(BF16)

        def down_plain(t, _):
            @pl.when((t == 2) & (b == 0))
            def _():
                finish_sum(1, 0, 0, n_down)

            @pl.when((t == 2) & (b == 1))
            def _():
                finish_sum(0, 1, 0, n_down)

            down(t, False)
            return 0

        def down_norm(t, _):
            down(t, True)
            return 0

        lax.fori_loop(0, 3, down_plain, 0)

        @pl.when(b == 0)
        def _():
            finish_wait(1, 0, 0, n_down)

        @pl.when(b == 1)
        def _():
            finish_wait(0, 1, 0, n_down)

        lax.fori_loop(3, n_down, down_norm, 0)
        send_part(b, 1, n_down - 1).start()
        chip_add(b, 1, n_down - 2)

    hidden_copies[0].start()
    raw_start(w_query, 0)
    hidden_copies[1].start()
    barrier = pltpu.get_barrier_semaphore()
    for device in (peer, far):
        pl.semaphore_signal(barrier, inc=1, device_id=device, device_id_type=pl.DeviceIdType.MESH)
    for i in range(n_layers):
        gains[pl.ds(2 * i, 1), :] = gain_attn[pl.ds(i, 1), :]
        gains[pl.ds(2 * i + 1, 1), :] = gain_mlp[pl.ds(i, 1), :]
    hidden_copies[0].wait()
    pl.semaphore_wait(barrier, 2)

    def layer_step(layer, _):
        def attn_step(b, _):
            attn_phase(layer, b)
            return 0

        def mlp_step(b, _):
            mlp_phase(layer, b)
            return 0

        lax.fori_loop(0, prompts, attn_step, 0)
        lax.fori_loop(0, prompts, mlp_step, 0)
        return 0

    lax.fori_loop(0, n_layers, layer_step, 0)
    out_copies = [pltpu.make_async_copy(x.at[b], out, x_sem.at[b]) for b, out in enumerate((h_out0, h_out1))]
    out_copies[0].start()
    chip_add(1, 1, n_down - 1)
    finish_sum(1, 1, 0, n_down)
    finish_wait(1, 1, 0, n_down)
    out_copies[1].start()
    for b in range(prompts):
        pl.semaphore_wait(credit.at[b], 1)
    wait(out_copies)


def solution(mesh):
    head_cols = P(None, None, "tp", None)
    head_rows = P(None, "tp", None, None)
    ff_cols = P(None, None, "tp")
    ff_rows = P(None, "tp", None)

    def shard_body(hidden, lengths, w_query, w_key, w_value, w_out, w_gate, w_up, w_down, norm_attn, norm_mlp):
        n_layers, model, heads, dim = w_query.shape
        prompts, seq, _ = hidden.shape
        width = w_gate.shape[2]
        inner = heads * dim
        n_down = model // TILE
        half = seq // 2
        cos_t, sin_t = rope_tables(seq, dim)
        anywhere = pl.BlockSpec(memory_space=pl.ANY)
        vmem = pl.BlockSpec(memory_space=pltpu.VMEM)
        dma = pltpu.SemaphoreType.DMA
        cache = jax.ShapeDtypeStruct((n_layers, prompts, heads, seq, dim), BF16)
        state = jax.ShapeDtypeStruct(hidden.shape[1:], BF16)
        h0, h1, k_cache, v_cache = pl.pallas_call(
            kernel,
            in_specs=[pl.BlockSpec(memory_space=pltpu.SMEM)] + [anywhere] * 8 + [vmem] * 4,
            out_specs=[anywhere] * 4,
            out_shape=[state, state, cache, cache],
            scratch_shapes=[
                pltpu.VMEM((prompts, seq, model), BF16),
                pltpu.VMEM((seq, model), BF16),
                pltpu.VMEM((seq, width), BF16),
                pltpu.VMEM((SLOTS, model, TILE), BF16),
                pltpu.VMEM((SLOTS, model, TILE), BF16),
                pltpu.VMEM((model, heads, dim), BF16),
                pltpu.VMEM((prompts, seq, model), BF16),
                pltpu.VMEM((prompts, half, model), BF16),
                pltpu.VMEM((prompts, half, model), BF16),
                pltpu.VMEM((2 * n_layers, model), F32),
                dma((prompts,)), dma((SLOTS,)), dma((SLOTS,)), dma((4,)), dma((n_down,)), dma((heads,)), dma((heads,)),
                dma((prompts, n_down)), dma((prompts, n_down)), dma((prompts, n_down)), dma((prompts, n_down)),
                dma((prompts, n_down)), dma((prompts, n_down)), pltpu.SemaphoreType.REGULAR((prompts,)),
            ],
            compiler_params=pltpu.CompilerParams(
                collective_id=0, has_side_effects=True, vmem_limit_bytes=63 * 1024 * 1024
            ),
        )(
            lengths, hidden, w_query, w_key, w_value, w_out.reshape(n_layers, inner, model), w_gate, w_up, w_down,
            norm_attn, norm_mlp, cos_t, sin_t,
        )
        return jnp.stack([h0, h1]), k_cache, v_cache

    return jax.shard_map(
        shard_body,
        mesh=mesh,
        in_specs=(P("dp"), P("dp"), head_cols, head_cols, head_cols, head_rows, ff_cols, ff_cols, ff_rows, P(), P()),
        out_specs=(P("dp"), P(None, "dp", "tp"), P(None, "dp", "tp")),
        check_vma=False,
    )
```

```python
import jax
import jax.numpy as jnp
import numpy as np
from jax import lax
from jax.experimental import pallas as pl
from jax.experimental.pallas import tpu as pltpu
from jax.sharding import PartitionSpec as P

RMS_EPS = 1e-6
ROPE_BASE = 10000.0
TILE = 512
SLOTS = 3
NORM_ROWS = 64
ACT_ROWS = 16
SPREAD_ROWS = 176
F32, BF16 = jnp.float32, jnp.bfloat16


def rope_tables(seq_len, head_dim):
    half_dim = head_dim // 2
    inv_freq = np.float32(ROPE_BASE) ** (-np.arange(half_dim, dtype=np.float32) * np.float32(2.0 / head_dim))
    angles = np.arange(seq_len, dtype=np.float32)[:, None] * inv_freq[None, :].astype(np.float32)
    return np.cos(angles).astype(np.float32), np.sin(angles).astype(np.float32)


def block(i, size):
    return pl.ds(pl.multiple_of(i * size, size), size)


def kernel(
    len_ref, hidden, w_query, w_key, w_value, w_out, w_gate, w_up, w_down, gain_attn, gain_mlp, cos_ref, sin_ref,
    h_out0, h_out1, k_cache, v_cache,
    x, a, m, wa, wb, raw, part, recv1, recv2, gains,
    x_sem, wa_sem, wb_sem, raw_sem, wo_sem, kc_sem, vc_sem, s1, r1, s2, r2, s3, r3, credit,
):
    n_layers, model, heads, dim = w_query.shape
    prompts, seq, _ = hidden.shape
    inner = heads * dim
    n_gu = w_gate.shape[2] // TILE
    n_down = model // TILE
    half = seq // 2
    n_raw = raw_sem.shape[0]
    raw_rows = model // n_raw
    half_dim = dim // 2

    me = lax.axis_index("tp")
    core = lax.rem(me, 2)
    peer = {"tp": me + 1 - 2 * core}
    far = {"tp": lax.rem(me + 2, 4)}
    own_row = core * half
    other_row = (1 - core) * half

    def rows_from(start, size):
        return pl.ds(pl.multiple_of(start, 128), size)

    def piece(stage, t):
        if stage == 0:
            j = lax.div(jnp.int32(t), 3)
            return j * (half // 2), half // 2, block(t - 3 * j, 2 * TILE)
        return 0, half, block(t, TILE)

    def remote(src, dst, send_sem, recv_sem, device):
        return pltpu.make_async_remote_copy(src, dst, send_sem, recv_sem, device_id=device, device_id_type=pl.DeviceIdType.MESH)

    def send_part(b, stage, t):
        row, n, c = piece(stage, t)
        return remote(
            part.at[b, rows_from(other_row + row, n), c], recv1.at[b, rows_from(row, n), c], s1.at[b, t], r1.at[b, t], peer
        )

    def send_far(b, stage, t):
        row, n, c = piece(stage, t)
        return remote(
            part.at[b, rows_from(own_row + row, n), c], recv2.at[b, rows_from(row, n), c],
            s2.at[b, t], r2.at[b, t], far,
        )

    def send_x(b, stage, t):
        row, n, c = piece(stage, t)
        rows = rows_from(own_row + row, n)
        return remote(x.at[b, rows, c], x.at[b, rows, c], s3.at[b, t], r3.at[b, t], peer)

    def chip_add(b, stage, t):
        row, n, c = piece(stage, t)
        rows = rows_from(own_row + row, n)
        send_part(b, stage, t).wait_recv()
        part[b, rows, c] = (part[b, rows, c].astype(F32) + recv1[b, rows_from(row, n), c].astype(F32)).astype(BF16)
        send_far(b, stage, t).start()

    def chip_adds(b, stage, first, last):
        def body(t, _):
            chip_add(b, stage, t)
            return 0

        lax.fori_loop(first, last, body, 0)

    def finish_sum(b, stage, first, last):
        def body(t, _):
            row, n, c = piece(stage, t)
            rows = rows_from(own_row + row, n)
            send_far(b, stage, t).wait_recv()
            total = part[b, rows, c].astype(F32) + recv2[b, rows_from(row, n), c].astype(F32)
            x[b, rows, c] = (x[b, rows, c].astype(F32) + total).astype(BF16)
            send_x(b, stage, t).start()
            return 0

        lax.fori_loop(first, last, body, 0)
        if last == n_down:
            pl.semaphore_signal(credit.at[b], inc=1, device_id=far, device_id_type=pl.DeviceIdType.MESH)

    def finish_wait(b, stage, first, last):
        def body(t, _):
            send_part(b, stage, t).wait_send()
            send_far(b, stage, t).wait_send()
            send_x(b, stage, t).wait()
            return 0

        lax.fori_loop(first, last, body, 0)

    def norm_rows(b, which, rows):
        v = x[b, rows, :].astype(F32)
        mean_sq = jnp.mean(v * v, axis=-1, keepdims=True)
        a[rows, :] = (v * lax.rsqrt(mean_sq + RMS_EPS) * (1.0 + gains[pl.ds(which, 1), :])).astype(BF16)

    def norm(b, which):
        def body(i, _):
            norm_rows(b, which, block(i, NORM_ROWS))
            return 0

        lax.fori_loop(0, seq // NORM_ROWS, body, 0)

    def raw_copy(w, layer, c):
        rows = pl.ds(c * raw_rows, raw_rows)
        return pltpu.make_async_copy(w.at[layer, rows], raw.at[rows], raw_sem.at[c])

    def raw_start(w, layer):
        for c in range(n_raw):
            raw_copy(w, layer, c).start()

    def relayout(slot, w, layer, then=None):
        for c in range(n_raw):
            raw_copy(w, layer, c).wait()
        for c in range(n_raw):
            rows = pl.ds(c * raw_rows, raw_rows)
            v = raw[rows].reshape(raw_rows, inner)
            wa[slot, rows, :] = v[:, :TILE]
            wb[slot, rows, :] = v[:, TILE:]
            if then is not None:
                raw_copy(then, layer, c).start()

    def out_copy(layer, t):
        dst = (wb if t % 2 else wa).at[2, pl.ds((t // 2) * inner, inner), :]
        return pltpu.make_async_copy(w_out.at[layer, :, pl.ds(t * TILE, TILE)], dst, wo_sem.at[t])

    def gu_copies(layer, t, slot):
        c = block(t, TILE)
        return (
            pltpu.make_async_copy(w_gate.at[layer, :, c], wa.at[slot], wa_sem.at[slot]),
            pltpu.make_async_copy(w_up.at[layer, :, c], wb.at[slot], wb_sem.at[slot]),
        )

    def down_copies(layer, t, slot):
        c = block(t, TILE)
        return (
            pltpu.make_async_copy(w_down.at[layer, pl.ds(0, model), c], wa.at[slot], wa_sem.at[slot]),
            pltpu.make_async_copy(w_down.at[layer, pl.ds(model, model), c], wb.at[slot], wb_sem.at[slot]),
        )

    def start(copies):
        for c in copies:
            c.start()

    def wait(copies):
        for c in copies:
            c.wait()

    def dot(p, q):
        return jnp.dot(p, q, preferred_element_type=F32)

    def cache_copies(layer, b, h):
        return (
            pltpu.make_async_copy(m.at[:, block(heads + h, dim)], k_cache.at[layer, b, h], kc_sem.at[h]),
            pltpu.make_async_copy(m.at[:, block(h, dim)], v_cache.at[layer, b, h], vc_sem.at[h]),
        )

    def rotate(v, first, scale):
        for r in range(0, seq, ACT_ROWS):
            rows = pl.ds(r, ACT_ROWS)
            cos_t, sin_t = cos_ref[rows, :], sin_ref[rows, :]
            for c in range(0, TILE, dim):
                lo, hi = v[r:r + ACT_ROWS, c:c + half_dim], v[r:r + ACT_ROWS, c + half_dim:c + dim]
                for d, w in ((0, lo * cos_t - hi * sin_t), (half_dim, hi * cos_t + lo * sin_t)):
                    w = w if scale is None else w * scale
                    m[rows, pl.ds(first + c + d, half_dim)] = w.astype(BF16)

    def head(b, i, j):
        h = 2 * i + j
        q = m[:, block(3 * heads + h, dim)]
        k = m[:, block(heads + h, dim)]
        for r in range(2):
            keys = (r + 1) * half
            v = m[pl.ds(0, keys), block(h, dim)]
            scores = lax.dot_general(q[r * half:keys], k[:keys], (((1,), (1,)), ((), ())), preferred_element_type=F32)
            row = r * half + lax.broadcasted_iota(jnp.int32, (half, keys), 0)
            col = lax.broadcasted_iota(jnp.int32, (half, keys), 1)
            scores = jnp.where((col <= row) & (col < len_ref[b]), scores, -1e30)
            p = jnp.exp(scores - jnp.max(scores, axis=-1, keepdims=True))
            p = (p * (1.0 / jnp.sum(p, axis=-1, keepdims=True))).astype(BF16)
            m[pl.ds(r * half, half), block(2 * heads + h, dim)] = dot(p, v).astype(BF16)

    hidden_copies = [pltpu.make_async_copy(hidden.at[b], x.at[b], x_sem.at[b]) for b in range(prompts)]

    def attn_phase(layer, b):
        @pl.when((layer == 0) & (b == 1))
        def _():
            hidden_copies[1].wait()

        @pl.when((layer == 0) | (b == 1))
        def _():
            norm(b, 2 * layer)

        @pl.when(b == 1)
        def _():
            chip_adds(0, 0, 2, n_down)

        relayout(0, w_query, layer, w_key)
        rotate(dot(a[...], wa[0]), 3 * inner, dim ** -0.5)
        rotate(dot(a[...], wb[0]), 3 * inner + TILE, dim ** -0.5)

        @pl.when((b == 0) & (layer > 0))
        def _():
            chip_add(1, 1, n_down - 1)

        relayout(1, w_key, layer, w_value)
        rotate(dot(a[...], wa[1]), inner, None)
        rotate(dot(a[...], wb[1]), inner + TILE, None)
        for t in range(n_down):
            out_copy(layer, t).start()
        relayout(0, w_value, layer)
        m[:, pl.ds(0, TILE)] = dot(a[...], wa[0]).astype(BF16)
        m[:, pl.ds(TILE, TILE)] = dot(a[...], wb[0]).astype(BF16)

        @pl.when(b == 0)
        def _():
            raw_start(w_query, layer)

        @pl.when(b == 1)
        def _():
            start(gu_copies(layer, 0, 0))
            start(gu_copies(layer, 1, 1))

        def two_heads(i, _):
            head(b, i, 0)
            head(b, i, 1)
            start(cache_copies(layer, b, 2 * i))
            start(cache_copies(layer, b, 2 * i + 1))
            return 0

        lax.fori_loop(0, heads // 2, two_heads, 0)

        @pl.when((b == 0) & (layer > 0))
        def _():
            finish_sum(1, 1, 0, n_down)

        for t in range(n_down):
            out_copy(layer, t).wait()
        o_cols = pl.ds(2 * inner, inner)

        def send_both(i):
            send_part(b, 0, i).start()
            send_part(b, 0, i + 3).start()

        def project(i, _):
            @pl.when(i > 0)
            def _():
                send_both(i - 1)

            part[b, :, block(2 * i, TILE)] = dot(m[:, o_cols], wa[2, block(i, inner), :]).astype(BF16)
            part[b, :, block(2 * i + 1, TILE)] = dot(m[:, o_cols], wb[2, block(i, inner), :]).astype(BF16)
            return 0

        lax.fori_loop(0, 3, project, 0)
        for h in range(heads):
            wait(cache_copies(layer, b, h))
        send_both(2)

        @pl.when(layer > 0)
        def _():
            pl.semaphore_wait(credit.at[b], 1)

        chip_adds(b, 0, 0, 2)

        @pl.when((b == 0) & (layer > 0))
        def _():
            finish_wait(1, 1, 0, n_down)

    def mlp_phase(layer, b):
        @pl.when((b == 1) & (layer + 1 < n_layers))
        def _():
            raw_start(w_query, layer + 1)

        def gate_up(u, steps, tile, h):
            slot, ahead = lax.rem(u, SLOTS), u + 2
            slot_ahead = lax.rem(ahead, SLOTS)
            t = tile(u)
            wait(gu_copies(layer, t, slot))

            @pl.when(ahead < steps)
            def _():
                start(gu_copies(layer, tile(ahead), slot_ahead))

            @pl.when(ahead >= steps)
            def _():
                start(down_copies(layer, ahead - steps, slot_ahead))

            if h is None:
                lhs = a[...]
                starts = range(0, seq, ACT_ROWS)
            else:
                quarter = half // 2
                lows = [rows_from(i * half + h * quarter, quarter) for i in range(2)]
                lhs = jnp.concatenate([a[r, :] for r in lows], axis=0)
                starts = [i * half + h * quarter + r for i in range(2) for r in range(0, quarter, ACT_ROWS)]
            gate = dot(lhs, wa[slot])
            up = dot(lhs, wb[slot])
            for i, row in enumerate(starts):
                r = i * ACT_ROWS
                act = jax.nn.gelu(gate[r:r + ACT_ROWS], approximate=True) * up[r:r + ACT_ROWS]
                m[pl.ds(row if h is None else pl.multiple_of(row, ACT_ROWS), ACT_ROWS), block(t, TILE)] = act.astype(BF16)

        def norm_half(h):
            def body(i, _):
                j = lax.div(i, 2)
                norm_rows(0, 2 * layer + 1, pl.ds(pl.multiple_of(j * half + h * (half // 2) + (i - 2 * j) * NORM_ROWS, NORM_ROWS), NORM_ROWS))
                return 0

            lax.fori_loop(0, 4, body, 0)

        @pl.when(b == 0)
        def _():
            finish_sum(0, 0, 0, 3)
            chip_adds(1, 0, 2, n_down)
            finish_wait(0, 0, 0, 3)
            norm_half(0)

            split = 3 * n_gu // 4
            steps = n_gu + split

            def tile(u):
                group = lax.div(u - split, 4)
                late = u - split - 4 * group
                return jnp.where(u < split, u, jnp.where(late < 3, 3 * group + late, split + group))

            def step(u, _):
                whole = (u >= split) & (lax.rem(u - split + 4, 4) == 3)

                @pl.when(u == split - 1)
                def _():
                    finish_sum(0, 0, 3, n_down)

                @pl.when(u == split)
                def _():
                    finish_wait(0, 0, 3, n_down)
                    norm_half(1)

                @pl.when(jnp.logical_not(whole))
                def _():
                    gate_up(u, steps, tile, jnp.where(u < split, 0, 1))

                @pl.when(whole)
                def _():
                    gate_up(u, steps, tile, None)

                return 0

            lax.fori_loop(0, steps, step, 0)

        @pl.when(b == 1)
        def _():
            def step(t, _):
                @pl.when(t == 1)
                def _():
                    chip_add(0, 1, n_down - 1)

                gate_up(t, n_gu, lambda u: u, None)
                return 0

            lax.fori_loop(0, n_gu, step, 0)

        next_norm = jnp.minimum(2 * layer + 1 + b, 2 * n_layers - 1)

        def down(t, with_norm):
            slot, ahead = lax.rem(t, SLOTS), t + 2
            slot_ahead = lax.rem(ahead, SLOTS)
            wait(down_copies(layer, t, slot))

            @pl.when(ahead < n_down)
            def _():
                start(down_copies(layer, ahead, slot_ahead))

            @pl.when((ahead >= n_down) & (b == 0))
            def _():
                start(gu_copies(layer, ahead - n_down, slot_ahead))

            @pl.when(t > 0)
            def _():
                send_part(b, 1, t - 1).start()

            @pl.when(t == 2)
            def _():
                pl.semaphore_wait(credit.at[b], 1)

            @pl.when(t > 1)
            def _():
                chip_add(b, 1, t - 2)

            if with_norm:
                first = jnp.minimum((t - 3) * SPREAD_ROWS, seq - SPREAD_ROWS)
                for r in range(0, SPREAD_ROWS, ACT_ROWS):
                    norm_rows(1 - b, next_norm, pl.ds(pl.multiple_of(first + r, ACT_ROWS), ACT_ROWS))
            part[b, :, block(t, TILE)] = (
                dot(m[:, pl.ds(0, model)], wa[slot]) + dot(m[:, pl.ds(model, model)], wb[slot])
            ).astype(BF16)

        def down_plain(t, _):
            @pl.when((t == 2) & (b == 0))
            def _():
                finish_sum(1, 0, 0, n_down)

            @pl.when((t == 2) & (b == 1))
            def _():
                finish_sum(0, 1, 0, n_down)

            down(t, False)
            return 0

        def down_norm(t, _):
            down(t, True)
            return 0

        lax.fori_loop(0, 3, down_plain, 0)

        @pl.when(b == 0)
        def _():
            finish_wait(1, 0, 0, n_down)

        @pl.when(b == 1)
        def _():
            finish_wait(0, 1, 0, n_down)

        lax.fori_loop(3, n_down, down_norm, 0)
        send_part(b, 1, n_down - 1).start()
        chip_add(b, 1, n_down - 2)

    hidden_copies[0].start()
    raw_start(w_query, 0)
    hidden_copies[1].start()
    barrier = pltpu.get_barrier_semaphore()
    for device in (peer, far):
        pl.semaphore_signal(barrier, inc=1, device_id=device, device_id_type=pl.DeviceIdType.MESH)
    for i in range(n_layers):
        gains[pl.ds(2 * i, 1), :] = gain_attn[pl.ds(i, 1), :]
        gains[pl.ds(2 * i + 1, 1), :] = gain_mlp[pl.ds(i, 1), :]
    hidden_copies[0].wait()
    pl.semaphore_wait(barrier, 2)

    def layer_step(layer, _):
        def attn_step(b, _):
            attn_phase(layer, b)
            return 0

        def mlp_step(b, _):
            mlp_phase(layer, b)
            return 0

        lax.fori_loop(0, prompts, attn_step, 0)
        lax.fori_loop(0, prompts, mlp_step, 0)
        return 0

    lax.fori_loop(0, n_layers, layer_step, 0)
    out_copies = [pltpu.make_async_copy(x.at[b], out, x_sem.at[b]) for b, out in enumerate((h_out0, h_out1))]
    out_copies[0].start()
    chip_add(1, 1, n_down - 1)
    finish_sum(1, 1, 0, n_down)
    finish_wait(1, 1, 0, n_down)
    out_copies[1].start()
    for b in range(prompts):
        pl.semaphore_wait(credit.at[b], 1)
    wait(out_copies)


def solution(mesh):
    head_cols = P(None, None, "tp", None)
    head_rows = P(None, "tp", None, None)
    ff_cols = P(None, None, "tp")
    ff_rows = P(None, "tp", None)

    def shard_body(hidden, lengths, w_query, w_key, w_value, w_out, w_gate, w_up, w_down, norm_attn, norm_mlp):
        n_layers, model, heads, dim = w_query.shape
        prompts, seq, _ = hidden.shape
        width = w_gate.shape[2]
        inner = heads * dim
        n_down = model // TILE
        half = seq // 2
        cos_t, sin_t = rope_tables(seq, dim)
        anywhere = pl.BlockSpec(memory_space=pl.ANY)
        vmem = pl.BlockSpec(memory_space=pltpu.VMEM)
        dma = pltpu.SemaphoreType.DMA
        cache = jax.ShapeDtypeStruct((n_layers, prompts, heads, seq, dim), BF16)
        state = jax.ShapeDtypeStruct(hidden.shape[1:], BF16)
        h0, h1, k_cache, v_cache = pl.pallas_call(
            kernel,
            in_specs=[pl.BlockSpec(memory_space=pltpu.SMEM)] + [anywhere] * 8 + [vmem] * 4,
            out_specs=[anywhere] * 4,
            out_shape=[state, state, cache, cache],
            scratch_shapes=[
                pltpu.VMEM((prompts, seq, model), BF16),
                pltpu.VMEM((seq, model), BF16),
                pltpu.VMEM((seq, width), BF16),
                pltpu.VMEM((SLOTS, model, TILE), BF16),
                pltpu.VMEM((SLOTS, model, TILE), BF16),
                pltpu.VMEM((model, heads, dim), BF16),
                pltpu.VMEM((prompts, seq, model), BF16),
                pltpu.VMEM((prompts, half, model), BF16),
                pltpu.VMEM((prompts, half, model), BF16),
                pltpu.VMEM((2 * n_layers, model), F32),
                dma((prompts,)), dma((SLOTS,)), dma((SLOTS,)), dma((4,)), dma((n_down,)), dma((heads,)), dma((heads,)),
                dma((prompts, n_down)), dma((prompts, n_down)), dma((prompts, n_down)), dma((prompts, n_down)),
                dma((prompts, n_down)), dma((prompts, n_down)), pltpu.SemaphoreType.REGULAR((prompts,)),
            ],
            compiler_params=pltpu.CompilerParams(
                collective_id=0, has_side_effects=True, vmem_limit_bytes=63 * 1024 * 1024
            ),
        )(
            lengths, hidden, w_query, w_key, w_value, w_out.reshape(n_layers, inner, model), w_gate, w_up, w_down,
            norm_attn, norm_mlp, cos_t, sin_t,
        )
        return jnp.stack([h0, h1]), k_cache, v_cache

    return jax.shard_map(
        shard_body,
        mesh=mesh,
        in_specs=(P("dp"), P("dp"), head_cols, head_cols, head_cols, head_rows, ff_cols, ff_cols, ff_rows, P(), P()),
        out_specs=(P("dp"), P(None, "dp", "tp"), P(None, "dp", "tp")),
        check_vma=False,
    )
```
